32 devices in a mesh: band: 16 (over z, y, core), grid: 2 (over x).
Axes of the slice: x: 2, y: 2, z: 4, core: 2. Of those that a mesh axis runs over, the one named last changes fastest.
Arguments:
- orbitals: float32 [32, 64, 4096], P('band', 'grid'), may hold values from -4 to 4
- pair_list: int32 [16, 4, 2], P('band'), may hold values from 0 to 31, as said below
- pair_count: int32 [16], P('band'), may hold values from 1 to 4, 32 in all
Outputs:
- exchange_proj: float32 [32, 64, 4096], P('band', 'grid')
The draws below stay inside these ranges and needn't reach their ends.
Inputs may be any that keep to these rules, and one draw needn't show every extreme that they name: `pair_list`: entry 0 is an orbital index 0 to 1 within the row's band group; entry 1 is a global orbital index owned by the same band group or by one of the next 2 groups, counted cyclically; the two never name the same orbital. Band group b uses its first pair_count[b] slots.
All inputs are finite; a program needn't handle non-finite values.
Results may differ from the reference program's by a relative error of at most 0.0003.
Values sent between devices are 32-bit elements; how exact they have to be, the bound alone decides.
A program may use at most 64 MiB of HBM per device.

```python
import math
import jax
import jax.numpy as jnp
import numpy as np
from jax import lax

CELL_SPAN_COUNT = 64
ORB_DEV = 2
PAIR_MEAN = 2
REACH = 2
SLOTS = 4
NORB = 32
N_BAND = 16


def draw_orbitals(key, part):
    lattice_position = jnp.arange(CELL_SPAN_COUNT).astype(jnp.float32)
    spread = CELL_SPAN_COUNT / 4.0

    def single(number):
        folded = jax.random.fold_in(jax.random.fold_in(key, 7001), number)
        key_centre, key_wave, key_phase, key_rough = jax.random.split(folded, 4)
        centre = jax.random.uniform(key_centre, (3,), minval=0.0, maxval=float(CELL_SPAN_COUNT))
        offsets = jnp.abs(lattice_position[None, :] - centre[:, None])
        offsets = jnp.minimum(offsets, CELL_SPAN_COUNT - offsets)
        radius = offsets[0][:, None, None] ** 2 + offsets[1][None, :, None] ** 2 + offsets[2][None, None, :] ** 2
        bell_shaped_decay = jnp.exp(-radius / (2.0 * spread * spread))
        fourier_modes = jax.random.randint(key_wave, (3,), 2, CELL_SPAN_COUNT * 5 // 16 + 1).astype(jnp.float32)
        angular_displacements = jax.random.uniform(key_phase, (3,), minval=0.0, maxval=2.0 * math.pi)
        oscillating_sinusoids = jnp.cos(fourier_modes[:, None] * lattice_position[None, :] * (2.0 * math.pi / CELL_SPAN_COUNT) + angular_displacements[:, None])
        oscillating_sinusoid = oscillating_sinusoids[0][:, None, None] * oscillating_sinusoids[1][None, :, None] * oscillating_sinusoids[2][None, None, :]
        random_perturbation = jnp.clip(0.5 * jax.random.normal(key_rough, (CELL_SPAN_COUNT, CELL_SPAN_COUNT, CELL_SPAN_COUNT)), -0.9, 0.9)
        electron_function_samples = jnp.clip(2.5 * bell_shaped_decay * (oscillating_sinusoid + 0.45 * random_perturbation), -4.0, 4.0)
        return electron_function_samples.reshape(CELL_SPAN_COUNT, CELL_SPAN_COUNT * CELL_SPAN_COUNT).astype(jnp.float32)
    return lax.map(single, jnp.arange(NORB))


def draw_pair_list(key, part):
    groups = NORB // ORB_DEV
    key_first, key_hop, key_partner = jax.random.split(jax.random.fold_in(key, 7002), 3)
    first_index = jax.random.randint(key_first, (groups, SLOTS), 0, ORB_DEV)
    hop_count = jax.random.randint(key_hop, (groups, SLOTS), 0, REACH + 1)
    partner = jax.random.randint(key_partner, (groups, SLOTS), 0, ORB_DEV)
    partner = jnp.where((hop_count == 0) & (partner == first_index), (first_index + 1) % ORB_DEV, partner)
    group_ids = jnp.arange(groups, dtype=jnp.int32)[:, None]
    global_partner = (group_ids + hop_count) % groups * ORB_DEV + partner
    return jnp.stack([first_index, global_partner], axis=-1).astype(jnp.int32)


def split_up(amount, total, bound, slope):
    portions = [(1 << 20) // math.isqrt(standing ** slope) + 1 for standing in range(2, amount + 1)]
    surplus, given = total - bound - (amount - 1), [1] * (amount - 1)
    while surplus > 0:
        movable = [i for i in range(amount - 1) if given[i] < bound]
        mass, budget = sum([portions[i] for i in movable]), surplus
        for i in movable:
            addition = min(bound - given[i], max(1, budget * portions[i] // mass), surplus)
            given[i] = given[i] + addition
            surplus = surplus - addition
    return np.array([bound] + given)


def ragged_sizes(own_key, count, total, reach, skew):
    if count == 2:
        one = jax.random.randint(own_key, (), max(1, total - reach), min(reach, total - 1) + 1)
        return jnp.stack([one, total - one])
    sizes = jnp.asarray(split_up(count, total, reach, skew), jnp.int32)
    pairs = (count - 1) // 2
    source_of, receiver = sizes[1:1 + 2 * pairs:2], sizes[2:2 + 2 * pairs:2]
    margin = jnp.minimum(source_of - 1, reach - receiver)
    shifted = jax.random.randint(jax.random.fold_in(own_key, 1), (pairs,), 0, 1 << 20) % (margin + 1)
    sizes = sizes.at[1:1 + 2 * pairs:2].set(source_of - shifted).at[2:2 + 2 * pairs:2].set(receiver + shifted)
    return sizes[jax.random.permutation(jax.random.fold_in(own_key, 2), count)]


def setup_inputs(seed: int = 0) -> dict:
    key_of = jax.random.split(jax.random.key(seed), 4)
    return {
        "orbitals": draw_orbitals(jax.random.fold_in(key_of[3], 71), 0),
        "pair_list": draw_pair_list(jax.random.fold_in(key_of[3], 71), 0),
        "pair_count": ragged_sizes(key_of[2], N_BAND, PAIR_MEAN * N_BAND, SLOTS, 2).astype(jnp.int32),
    }


def kernel_table():
    points = jnp.arange(CELL_SPAN_COUNT).astype(jnp.float32)
    eigenvalues = 2.0 - 2.0 * jnp.cos(points * (2.0 * math.pi / CELL_SPAN_COUNT))
    summed = eigenvalues[:, None, None] + eigenvalues[None, :, None] + eigenvalues[None, None, :]
    return (1.0 / CELL_SPAN_COUNT) / (1.0 / CELL_SPAN_COUNT ** 2 + summed)


def reference(orbitals, pair_list, pair_count):
    groups = pair_list.shape[0]
    slot_count = pair_list.shape[1]
    kernel = kernel_table()
    group_ids = jnp.repeat(jnp.arange(groups, dtype=jnp.int32), slot_count)
    flat = pair_list.reshape(-1, 2).astype(jnp.int32)
    first_index = (group_ids * ORB_DEV + flat[:, 0]).astype(jnp.int32)
    second = flat[:, 1].astype(jnp.int32)
    alive = (jnp.arange(slot_count)[None, :] < pair_count[:, None]).reshape(-1).astype(orbitals.dtype)

    def visit(totals, inputs):
        left_id, right_id, weight = inputs
        left_rows = orbitals[left_id]
        right_rows = orbitals[right_id]
        density = (left_rows * right_rows * weight).reshape(CELL_SPAN_COUNT, CELL_SPAN_COUNT, CELL_SPAN_COUNT)
        spectrum = jnp.fft.fftn(density) * kernel
        potential = jnp.real(jnp.fft.ifftn(spectrum)).astype(density.dtype).reshape(CELL_SPAN_COUNT, CELL_SPAN_COUNT * CELL_SPAN_COUNT)
        totals = totals.at[left_id].add(potential * right_rows)
        totals = totals.at[right_id].add(potential * left_rows)
        return totals, None

    totals, unused = lax.scan(visit, jnp.zeros(orbitals.shape, orbitals.dtype), (first_index, second, alive))
    return totals
```

```python
import functools
import math

import jax
import jax.numpy as jnp
import numpy as np
from jax import lax
from jax.experimental import pallas as pl
from jax.experimental.pallas import tpu as pltpu
from jax.sharding import PartitionSpec as P

REACH = 2
GROUP = 8


def rotated(value, axis, steps):
    count = lax.axis_size(axis)
    pairs = [(source, (source + steps) % count) for source in range(count)]
    return lax.ppermute(value, axis, pairs)


def swapped(value, axis):
    count = lax.axis_size(axis)
    return lax.ppermute(value, axis, [(source, source ^ 1) for source in range(count)])


def split(value):
    high = value.astype(jnp.bfloat16)
    return high, (value - high.astype(jnp.float32)).astype(jnp.bfloat16)


def tables(side, half_rows):
    points = np.arange(side)
    angles = (points[:, None] * points[None, :] % side) * (2.0 * math.pi / side)
    hartley = (np.cos(angles) + np.sin(angles)).astype(np.float32)
    high = hartley.astype(jnp.bfloat16)
    low = (hartley - high.astype(np.float32)).astype(jnp.bfloat16)
    eye = np.eye(2, dtype=np.float32)
    wide_high = np.kron(eye, high.astype(np.float32))
    wide_low = np.kron(eye, low.astype(np.float32))
    right = np.block([[wide_high, wide_low], [wide_high, wide_low]]).astype(jnp.bfloat16)
    left = np.concatenate([high, high, low], 1)
    eigenvalues = 2.0 - 2.0 * np.cos(points * (2.0 * math.pi / side))
    shift = 1.0 / side**2 + eigenvalues[:, None] + np.tile(eigenvalues, 2)[None, :]
    ratio = 1.0 + shift / 2 - np.sqrt(shift + shift**2 / 4)
    power = ratio**half_rows
    reach = ratio**GROUP
    scale = 1.0 / side / (1.0 / ratio - ratio) / side**2
    wrap = 1.0 / (1.0 - power**4)
    decay = np.stack([ratio, power, scale, wrap, reach]).astype(np.float32)
    return right, left, decay


def along_last(value, right):
    width = value.shape[1]
    product = jnp.dot(
        jnp.concatenate(split(value), 1), right, preferred_element_type=jnp.float32
    )
    return product[:, :width] + product[:, width:]


def along_second(planes, left):
    width = planes[0].shape[1]
    out = []
    for start in range(0, len(planes), 2):
        both = jnp.concatenate(planes[start : start + 2], 1)
        high, low = split(both)
        stacked = jnp.concatenate([high, low, high], 0)
        product = jnp.dot(left, stacked, preferred_element_type=jnp.float32)
        out.append(product[:, :width])
        out.append(product[:, width:])
    return out


def halves(value):
    return pltpu.roll(value, value.shape[-1] // 2, axis=value.ndim - 1)


def arrange_kernel(index, after, source, chunk):
    owned, slab_rows, cells = source.shape
    width = chunk.shape[-1]
    lower = lax.broadcasted_iota(jnp.int32, (GROUP, width), 1) < width // 2
    tiles = 4

    def tile_step(step, carry):
        for row in range(owned):
            lines = []
            for k in range(tiles):
                lanes = pl.ds(pl.multiple_of((step * tiles + k) * width, width), width)
                near = source[row, pl.ds(index * GROUP, GROUP), lanes]
                far = source[row, pl.ds(index * GROUP + slab_rows // 2, GROUP), lanes]
                lines.append(jnp.where(lower, near, halves(far)))
                lines.append(jnp.where(lower, halves(near), far))
            block = jnp.swapaxes(jnp.stack(lines, 0), 0, 1)
            chunk[row, :, pl.ds(pl.multiple_of(step * 2 * tiles, 2 * tiles), 2 * tiles), :] = block
        return carry

    lax.fori_loop(0, cells // (width * tiles), tile_step, 0)


def restore_kernel(flag, *refs):
    out = refs[-1]
    count = (len(refs) - 1) // 3
    own, passed, arrived = refs[:count], refs[count : 2 * count], refs[2 * count : -1]
    owned, slab_rows, cells = out.shape
    width = own[0].shape[-1]
    lower = lax.broadcasted_iota(jnp.int32, (GROUP, width), 1) < width // 2
    weight = flag[0].astype(jnp.float32)
    tiles = 4

    def tile_step(step, carry):
        ys = pl.ds(pl.multiple_of(step * 2 * tiles, 2 * tiles), 2 * tiles)
        for row in range(owned):
            for c in range(count):
                block = (
                    own[c][row, :, ys, :]
                    + weight * passed[c][row, :, ys, :]
                    + arrived[c][row, :, ys, :]
                )
                block = jnp.swapaxes(block, 0, 1)
                for k in range(tiles):
                    lanes = pl.ds(pl.multiple_of((step * tiles + k) * width, width), width)
                    even, odd = block[2 * k], block[2 * k + 1]
                    out[row, pl.ds(c * GROUP, GROUP), lanes] = jnp.where(
                        lower, even, halves(odd)
                    )
                    out[row, pl.ds(c * GROUP + slab_rows // 2, GROUP), lanes] = jnp.where(
                        lower, halves(even), odd
                    )
        return carry

    lax.fori_loop(0, cells // (width * tiles), tile_step, 0)


def pick_kernel(flag, after, far, own, out):
    @pl.when(flag[0] == 0)
    def _():
        out[...] = far[...]

    @pl.when(flag[0] == 1)
    def _():
        out[...] = own[...]


def join_kernel(flag, after, distant, handed, out):
    weight = 1.0 - flag[0].astype(jnp.float32)
    out[...] = distant[...] + weight * handed[...]


def forward_kernel(chosen, after, own, near, far, right_ref, left_ref, decay, spectrum, moments, window):
    slots, rows, side, width = spectrum.shape
    owned = own.shape[0]
    window[:owned] = own[...]
    window[owned : 2 * owned] = near[...]
    window[2 * owned :] = far[...]
    right = right_ref[...]
    left = left_ref[...]

    def slot_step(slot, carry):
        first = chosen[0, slot]
        second = chosen[1, slot]
        density = window[first] * window[second]
        value = along_last(density.reshape(rows * side, width), right)
        planes = [value[k * side : (k + 1) * side] for k in range(rows)]
        planes = along_second(planes, left)
        ratio = decay[0]
        ahead = planes[0]
        behind = planes[-1]
        for k in range(rows):
            spectrum[slot, k] = planes[k]
            if k:
                ahead = ahead * ratio + planes[k]
                behind = behind * ratio + planes[rows - 1 - k]
        moments[slot, 0] = ahead
        moments[slot, 1] = behind
        return carry

    lax.fori_loop(0, chosen[2, 0], slot_step, 0)


def packed_moments(moments, decay):
    power, reach = decay[1], decay[4]
    ahead = moments[0][:, 0]
    behind = moments[-1][:, 1]
    for k in range(1, len(moments)):
        ahead = ahead * reach + moments[k][:, 0]
        behind = behind * reach + moments[-1 - k][:, 1]
    half = ahead.shape[-1] // 2
    ahead_slab = ahead[..., half:] + power[:, half:] * ahead[..., :half]
    behind_slab = behind[..., :half] + power[:, :half] * behind[..., half:]
    return jnp.concatenate([behind_slab, ahead_slab], -1)


def backward_kernel(index, count, chosen, after, older, sent, own, near, far, spectrum, *refs):
    moments = refs[:count]
    mine, other, right_ref, left_ref, decay, kept, handed, distant, window, out = refs[count:]
    slots, rows, side, width = spectrum.shape
    owned = own.shape[0]
    window[:owned] = own[...]
    window[owned : 2 * owned] = near[...]
    window[2 * owned :] = far[...]
    right = right_ref[...]
    left = left_ref[...]
    out[...] = jnp.zeros_like(out)
    lower = lax.broadcasted_iota(jnp.int32, (side, width), 1) < width // 2

    def slot_step(slot, carry):
        first = chosen[0, slot]
        second = chosen[1, slot]
        ratio, power, scale, wrap, reach = [decay[k] for k in range(5)]
        ahead_all = moments[0][slot, 0]
        behind_all = moments[-1][slot, 1]
        for k in range(1, count):
            ahead_all = ahead_all * reach + moments[k][slot, 0]
            behind_all = behind_all * reach + moments[-1 - k][slot, 1]
        entering = (other[slot] + power * power * mine[slot]) * wrap
        turned = halves(entering)
        ahead = jnp.where(lower, turned, halves(ahead_all) + power * entering)
        behind = jnp.where(lower, halves(behind_all) + power * entering, turned)
        for k in range(index):
            ahead = ahead * reach + moments[k][slot, 0]
        for k in reversed(range(index + 1, count)):
            behind = behind * reach + moments[k][slot, 1]
        tails = []
        for k in reversed(range(rows)):
            spilled = ratio * behind
            tails.insert(0, spilled)
            behind = spectrum[slot, k] + spilled
        planes = []
        for k in range(rows):
            ahead = spectrum[slot, k] + ratio * ahead
            planes.append(scale * (ahead + tails[k]))
        planes = along_second(planes, left)
        value = along_last(jnp.concatenate(planes, 0), right)
        potential = value.reshape(rows, side, width)
        out[first] += potential * window[second]
        out[second] += potential * window[first]
        return carry

    lax.fori_loop(0, chosen[2, 0], slot_step, 0)
    kept[...] = out[:owned]
    handed[...] = out[owned : 2 * owned]
    distant[...] = out[2 * owned :]


def on_device(orbitals, pair_list, pair_count):
    owned_rows, slab_rows, plane_cells = orbitals.shape
    side = math.isqrt(plane_cells)
    assert lax.axis_size("grid") == 2 and REACH == 2
    rows = slab_rows // 2
    count = rows // GROUP
    band_count = lax.axis_size("band")
    band_index = lax.axis_index("band")
    even = band_index % 2 == 0
    right, left, decay = tables(side, rows)
    smem = pl.BlockSpec(memory_space=pltpu.SMEM)
    vmem = pl.BlockSpec(memory_space=pltpu.VMEM)
    params = pltpu.CompilerParams(vmem_limit_bytes=12 * 2**20)
    shape = (owned_rows, GROUP, side, 2 * side)
    block = jax.ShapeDtypeStruct(shape, jnp.float32)
    whole = (3 * owned_rows,) + shape[1:]

    def cost(megabytes):
        return pl.CostEstimate(flops=0, bytes_accessed=megabytes << 20, transcendentals=0)

    fields, after = [], orbitals
    for c in range(count):
        after = pl.pallas_call(
            functools.partial(arrange_kernel, c),
            out_shape=block,
            in_specs=[vmem, vmem],
            out_specs=vmem,
            compiler_params=params,
            cost_estimate=cost(1),
            name="arrange",
        )(after, orbitals)
        fields.append(after)
    far = [rotated(field, "band", -2) for field in fields]
    flag = (band_index % 2).reshape(1)

    def near_block(index, after):
        picked = pl.pallas_call(
            pick_kernel,
            out_shape=block,
            in_specs=[smem, vmem, vmem, vmem],
            out_specs=vmem,
            compiler_params=params,
            cost_estimate=cost(1),
            name="pick",
        )(flag, after, far[index], fields[index])
        return swapped(picked, "band")

    near = [near_block(0, fields[0])]
    pair_rows = pair_list[0]
    slots = pair_rows.shape[0]
    partner = pair_rows[:, 1]
    distance = (partner // owned_rows - band_index) % band_count
    second = jnp.minimum(distance * owned_rows + partner % owned_rows, 3 * owned_rows - 1)
    chosen = jnp.stack(
        [pair_rows[:, 0], second, jnp.broadcast_to(pair_count[0], second.shape)]
    )
    spectra, moments = [], []
    for c in range(count):
        spectrum, moment = pl.pallas_call(
            forward_kernel,
            out_shape=(
                jax.ShapeDtypeStruct((slots,) + shape[1:], jnp.float32),
                jax.ShapeDtypeStruct((slots, 2, side, 2 * side), jnp.float32),
            ),
            in_specs=[smem] + [vmem] * 7,
            out_specs=(vmem, vmem),
            scratch_shapes=[pltpu.VMEM(whole, jnp.float32)],
            compiler_params=params,
            cost_estimate=cost(1),
            name="forward_planes",
        )(chosen, moments[-1] if c else fields[c], fields[c], near[c], far[c], right, left, decay)
        spectra.append(spectrum)
        moments.append(moment)
        if c + 1 < count:
            near.append(near_block(c + 1, moment))
    mine = packed_moments(moments, decay)
    other = swapped(mine, "grid")
    own, passed, joined, arrived = [], [], [], []
    for c in range(count):
        kept, handed, distant = pl.pallas_call(
            functools.partial(backward_kernel, c, count),
            out_shape=(block,) * 3,
            in_specs=[smem] + [vmem] * (12 + count),
            out_specs=(vmem,) * 3,
            scratch_shapes=[pltpu.VMEM(whole, jnp.float32)] * 2,
            compiler_params=params,
            cost_estimate=cost(1),
            name="backward_planes",
        )(
            chosen, own[-1] if c else mine, joined[c - 2] if c > 1 else mine,
            arrived[c - 3] if c > 2 else mine,
            fields[c], near[c], far[c], spectra[c], *moments,
            mine, other, right, left, decay,
        )
        handed = swapped(handed, "band")
        own.append(kept)
        passed.append(handed)
        total = pl.pallas_call(
            join_kernel,
            out_shape=block,
            in_specs=[smem] + [vmem] * 3,
            out_specs=vmem,
            compiler_params=params,
            cost_estimate=cost(1),
            name="join",
        )(flag, joined[-1] if c else kept, distant, handed)
        joined.append(total)
        arrived.append(rotated(joined[-1], "band", 2))
    return pl.pallas_call(
        restore_kernel,
        out_shape=jax.ShapeDtypeStruct(orbitals.shape, jnp.float32),
        in_specs=[smem] + [vmem] * (3 * count),
        out_specs=vmem,
        compiler_params=params,
        cost_estimate=cost(6),
        name="restore",
    )(flag, *own, *passed, *arrived)


def solution(mesh):
    in_specs = (P("band", "grid", None), P("band", None, None), P("band"))
    out_specs = P("band", "grid", None)
    return jax.shard_map(
        on_device, mesh=mesh, in_specs=in_specs, out_specs=out_specs, check_vma=False
    )
```

```python
import functools
import math

import jax
import jax.numpy as jnp
import numpy as np
from jax import lax
from jax.experimental import pallas as pl
from jax.experimental.pallas import tpu as pltpu
from jax.sharding import PartitionSpec as P

REACH = 2
GROUP = 8


def rotated(value, axis, steps):
    count = lax.axis_size(axis)
    pairs = [(source, (source + steps) % count) for source in range(count)]
    return lax.ppermute(value, axis, pairs)


def swapped(value, axis):
    count = lax.axis_size(axis)
    return lax.ppermute(value, axis, [(source, source ^ 1) for source in range(count)])


def split(value):
    high = value.astype(jnp.bfloat16)
    return high, (value - high.astype(jnp.float32)).astype(jnp.bfloat16)


def tables(side, half_rows):
    points = np.arange(side)
    angles = (points[:, None] * points[None, :] % side) * (2.0 * math.pi / side)
    hartley = (np.cos(angles) + np.sin(angles)).astype(np.float32)
    high = hartley.astype(jnp.bfloat16)
    low = (hartley - high.astype(np.float32)).astype(jnp.bfloat16)
    eye = np.eye(2, dtype=np.float32)
    wide_high = np.kron(eye, high.astype(np.float32))
    wide_low = np.kron(eye, low.astype(np.float32))
    right = np.block([[wide_high, wide_low], [wide_high, wide_low]]).astype(jnp.bfloat16)
    left = np.concatenate([high, high, low], 1)
    eigenvalues = 2.0 - 2.0 * np.cos(points * (2.0 * math.pi / side))
    shift = 1.0 / side**2 + eigenvalues[:, None] + np.tile(eigenvalues, 2)[None, :]
    ratio = 1.0 + shift / 2 - np.sqrt(shift + shift**2 / 4)
    power = ratio**half_rows
    reach = ratio**GROUP
    scale = 1.0 / side / (1.0 / ratio - ratio) / side**2
    wrap = 1.0 / (1.0 - power**4)
    decay = np.stack([ratio, power, scale, wrap, reach]).astype(np.float32)
    return right, left, decay


def along_last(value, right):
    width = value.shape[1]
    product = jnp.dot(
        jnp.concatenate(split(value), 1), right, preferred_element_type=jnp.float32
    )
    return product[:, :width] + product[:, width:]


def along_second(planes, left):
    width = planes[0].shape[1]
    out = []
    for start in range(0, len(planes), 2):
        both = jnp.concatenate(planes[start : start + 2], 1)
        high, low = split(both)
        stacked = jnp.concatenate([high, low, high], 0)
        product = jnp.dot(left, stacked, preferred_element_type=jnp.float32)
        out.append(product[:, :width])
        out.append(product[:, width:])
    return out


def halves(value):
    return pltpu.roll(value, value.shape[-1] // 2, axis=value.ndim - 1)


def arrange_kernel(row, source, *refs):
    packed = refs[-1]
    _, slab_rows, cells = source.shape
    width = packed.shape[-1]
    half = slab_rows // 2
    lower = lax.broadcasted_iota(jnp.int32, (GROUP, width), 1) < width // 2
    tiles = 4

    def tile_step(step, carry):
        ys = pl.ds(pl.multiple_of(step * 2 * tiles, 2 * tiles), 2 * tiles)
        for start in range(0, half, GROUP):
            lines = []
            for k in range(tiles):
                lanes = pl.ds(pl.multiple_of((step * tiles + k) * width, width), width)
                near = source[row, pl.ds(start, GROUP), lanes]
                far = source[row, pl.ds(start + half, GROUP), lanes]
                lines.append(jnp.where(lower, near, halves(far)))
                lines.append(jnp.where(lower, halves(near), far))
            packed[pl.ds(start, GROUP), ys, :] = jnp.swapaxes(jnp.stack(lines, 0), 0, 1)
        return carry

    lax.fori_loop(0, cells // (width * tiles), tile_step, 0)


def stack_kernel(first, second, own):
    own[0] = first[...]
    own[1] = second[...]


def restore_kernel(row, flag, own, passed, arrived, *refs):
    out = refs[-1]
    _, slab_rows, cells = out.shape
    width = own.shape[-1]
    half = slab_rows // 2
    lower = lax.broadcasted_iota(jnp.int32, (GROUP, width), 1) < width // 2
    weight = flag[0].astype(jnp.float32)
    tiles = 4

    def tile_step(step, carry):
        ys = pl.ds(pl.multiple_of(step * 2 * tiles, 2 * tiles), 2 * tiles)
        for start in range(0, half, GROUP):
            planes = pl.ds(start, GROUP)
            block = own[row, planes, ys, :] + weight * passed[planes, ys, :] + arrived[planes, ys, :]
            block = jnp.swapaxes(block, 0, 1)
            for k in range(tiles):
                lanes = pl.ds(pl.multiple_of((step * tiles + k) * width, width), width)
                even, odd = block[2 * k], block[2 * k + 1]
                out[0, planes, lanes] = jnp.where(lower, even, halves(odd))
                out[0, pl.ds(start + half, GROUP), lanes] = jnp.where(lower, halves(even), odd)
        return carry

    lax.fori_loop(0, cells // (width * tiles), tile_step, 0)


def pick_kernel(flag, after, far, own, out):
    @pl.when(flag[0] == 0)
    def _():
        out[...] = far[...]

    @pl.when(flag[0] == 1)
    def _():
        out[...] = own[...]


def join_kernel(flag, after, distant, handed, out):
    weight = 1.0 - flag[0].astype(jnp.float32)
    out[...] = distant[...] + weight * handed[...]


def slab_moments(moments, i, reach):
    count = moments.shape[1]
    ahead = moments[i, 0, 0]
    behind = moments[i, count - 1, 1]
    for k in range(1, count):
        ahead = ahead * reach + moments[i, k, 0]
        behind = behind * reach + moments[i, count - 1 - k, 1]
    return ahead, behind


def forward_kernel(base, counts, after, own, other, right_ref, left_ref, decay, spectrum, moments, mine):
    owned, rows, side, width = own.shape
    chunks = rows // GROUP
    lower = lax.broadcasted_iota(jnp.int32, (side, width), 1) < width // 2

    def orbital_step(i, carry):
        live = counts[base + i] > 0

        def chunk_step(c, carry):
            block = pl.ds(pl.multiple_of(c * GROUP, GROUP), GROUP)
            density = own[i, block] * other[block]
            value = along_last(density.reshape(GROUP * side, width), right_ref[...])
            planes = [value[k * side : (k + 1) * side] for k in range(GROUP)]
            planes = along_second(planes, left_ref[...])
            ratio = decay[0]
            ahead = planes[0]
            behind = planes[-1]
            for k in range(GROUP):
                spectrum[i, c * GROUP + k] = planes[k]
                if k:
                    ahead = ahead * ratio + planes[k]
                    behind = behind * ratio + planes[GROUP - 1 - k]
            moments[i, c, 0] = ahead
            moments[i, c, 1] = behind
            return carry

        lax.fori_loop(0, jnp.where(live, chunks, 0), chunk_step, 0)

        @pl.when(live)
        def _():
            power = decay[1]
            ahead, behind = slab_moments(moments, i, decay[4])
            mine[i] = jnp.where(lower, behind + power * halves(behind), ahead + power * halves(ahead))

        return carry

    lax.fori_loop(0, owned, orbital_step, 0)


def backward_kernel(
    base, inside, counts, after, own, other, spectrum, moments, mine, arrived,
    right_ref, left_ref, decay, *refs
):
    edge = refs[-1]
    if inside:
        before, total = refs[:2]
        total[...] = before[...]
    else:
        total, partner = refs[-3:-1]
        total[...] = refs[0][...] if len(refs) > 3 else jnp.zeros_like(total)
        partner[...] = jnp.zeros_like(partner)
    owned, rows, side, width = own.shape
    chunks = rows // GROUP
    lower = lax.broadcasted_iota(jnp.int32, (side, width), 1) < width // 2

    def orbital_step(i, carry):
        number = counts[base + i]

        @pl.when(number > 0)
        def _():
            power, reach = decay[1], decay[4]
            ahead_all, behind_all = slab_moments(moments, i, reach)
            entering = (arrived[i] + power * power * mine[i]) * decay[3]
            turned = halves(entering)
            ahead = jnp.where(lower, turned, halves(ahead_all) + power * entering)
            behind = jnp.where(lower, halves(behind_all) + power * entering, turned)
            edge[0, 0] = ahead
            edge[chunks - 1, 1] = behind
            for k in range(1, chunks):
                ahead = ahead * reach + moments[i, k - 1, 0]
                edge[k, 0] = ahead
                behind = behind * reach + moments[i, chunks - k, 1]
                edge[chunks - 1 - k, 1] = behind

        def chunk_step(c, carry):
            block = pl.ds(pl.multiple_of(c * GROUP, GROUP), GROUP)
            ratio = decay[0]
            scale = decay[2] * number.astype(jnp.float32)
            ahead = edge[c, 0]
            behind = edge[c, 1]
            tails = []
            for k in reversed(range(GROUP)):
                spilled = ratio * behind
                tails.insert(0, spilled)
                behind = spectrum[i, c * GROUP + k] + spilled
            planes = []
            for k in range(GROUP):
                ahead = spectrum[i, c * GROUP + k] + ratio * ahead
                planes.append(scale * (ahead + tails[k]))
            planes = along_second(planes, left_ref[...])
            value = along_last(jnp.concatenate(planes, 0), right_ref[...])
            potential = value.reshape(GROUP, side, width)
            total[i, block] += potential * other[block]
            if inside:
                total[1, block] += potential * own[i, block]
            else:
                partner[block] += potential * own[i, block]
            return carry

        lax.fori_loop(0, jnp.where(number > 0, chunks, 0), chunk_step, 0)
        return carry

    lax.fori_loop(0, owned, orbital_step, 0)


def pair_counts(pair_list, pair_count, owned, band_index, band_count):
    first, partner = pair_list[0, :, 0], pair_list[0, :, 1]
    live = jnp.arange(first.shape[0]) < pair_count[0]
    distance = (partner // owned - band_index) % band_count
    inside = (REACH * owned) * owned
    place = ((partner % owned) * REACH + distance - 1) * owned + first
    place = jnp.where(distance == 0, inside, place)
    places = jnp.arange(inside + owned)
    return jnp.sum(jnp.where(live[None, :] & (place[None, :] == places[:, None]), 1, 0), axis=1)


def on_device(orbitals, pair_list, pair_count):
    owned, slab_rows, plane_cells = orbitals.shape
    side = math.isqrt(plane_cells)
    assert lax.axis_size("grid") == 2 and REACH == 2 and owned == 2
    rows = slab_rows // 2
    chunks = rows // GROUP
    band_count = lax.axis_size("band")
    band_index = lax.axis_index("band")
    right, left, decay = tables(side, rows)
    smem = pl.BlockSpec(memory_space=pltpu.SMEM)
    vmem = pl.BlockSpec(memory_space=pltpu.VMEM)
    free = pl.BlockSpec(memory_space=pl.ANY)
    params = pltpu.CompilerParams(vmem_limit_bytes=12 * 2**20)
    shape = (rows, side, 2 * side)
    one = jax.ShapeDtypeStruct(shape, jnp.float32)
    both = jax.ShapeDtypeStruct((owned,) + shape, jnp.float32)

    def call(kernel, out_shape, in_specs, out_specs=vmem, scratch=(), aliases={}, grid=()):
        if isinstance(out_shape, tuple):
            out_specs = (vmem,) * len(out_shape)
        return pl.pallas_call(
            kernel,
            out_shape=out_shape,
            grid=grid,
            in_specs=in_specs,
            out_specs=out_specs,
            scratch_shapes=scratch,
            compiler_params=params,
            input_output_aliases=aliases,
            cost_estimate=pl.CostEstimate(flops=0, bytes_accessed=1 << 20, transcendentals=0),
        )

    fields, far = [], []
    for row in range(owned):
        field = call(
            functools.partial(arrange_kernel, row), one, [vmem] + [free] * row
        )(orbitals, *fields)
        fields.append(field)
        far.append(rotated(field, "band", -2))
    own = call(stack_kernel, both, [vmem, vmem])(*fields)
    flag = (band_index % 2).reshape(1)
    counts = pair_counts(pair_list, pair_count, owned, band_index, band_count)

    def forward(base, after, other):
        spectrum, moments, mine = call(
            functools.partial(forward_kernel, base),
            (
                both,
                jax.ShapeDtypeStruct((owned, chunks, 2) + shape[1:], jnp.float32),
                jax.ShapeDtypeStruct((owned,) + shape[1:], jnp.float32),
            ),
            [smem, free] + [vmem] * 5,
        )(counts, after, own, other, right, left, decay)
        return (other, spectrum, moments, mine, swapped(mine, "grid"))

    def backward(base, after, state, total, inside=False):
        return call(
            functools.partial(backward_kernel, base, inside),
            both if inside else (both, one),
            [smem, free] + [vmem] * (9 + len(total)),
            scratch=[pltpu.VMEM((chunks, 2) + shape[1:], jnp.float32)],
        )(counts, after, own, *state, right, left, decay, *total)

    inner_base = REACH * owned * owned
    inner = forward(inner_base, own, fields[1])
    after = inner[3]
    total, passed, arrived = (), [], []
    for row in range(owned):
        base = row * REACH * owned
        picked = call(pick_kernel, one, [smem, free, vmem, vmem])(
            flag, after, far[row], fields[row]
        )
        near = swapped(picked, "band")
        distant_state = forward(base + owned, picked, far[row])
        near_state = forward(base, distant_state[3], near)
        acc, handed = backward(base, near_state[3], near_state, total)
        handed_over = swapped(handed, "band")
        acc, distant = backward(base + owned, handed, distant_state, (acc,))
        total = (acc,)
        joined = call(join_kernel, one, [smem, free, vmem, vmem])(
            flag, distant, distant, handed_over
        )
        passed.append(handed_over)
        arrived.append(rotated(joined, "band", 2))
        after = joined
    total = backward(inner_base, after, inner, total, inside=True)
    out = jax.ShapeDtypeStruct(orbitals.shape, jnp.float32)
    result = None
    for row in range(owned):
        earlier = [] if result is None else [result]
        result = call(
            functools.partial(restore_kernel, row),
            out,
            [smem] + [vmem] * 3 + [free] * len(earlier),
            out_specs=pl.BlockSpec(
                (1,) + orbitals.shape[1:], functools.partial(lambda r, step: (r, 0, 0), row)
            ),
            grid=(1,),
            aliases={4: 0} if earlier else {},
        )(flag, total, passed[row], arrived[row], *earlier)
    return result


def solution(mesh):
    in_specs = (P("band", "grid", None), P("band", None, None), P("band"))
    out_specs = P("band", "grid", None)

    return jax.shard_map(
        on_device, mesh=mesh, in_specs=in_specs, out_specs=out_specs, check_vma=False
    )
```

```python
import functools
import math

import jax
import jax.numpy as jnp
import numpy as np
from jax import lax
from jax.experimental import pallas as pl
from jax.experimental.pallas import tpu as pltpu
from jax.sharding import PartitionSpec as P

REACH = 2
GROUP = 8


def rotated(value, axis, steps):
    count = lax.axis_size(axis)
    pairs = [(source, (source + steps) % count) for source in range(count)]
    return lax.ppermute(value, axis, pairs)


def swapped(value, axis):
    count = lax.axis_size(axis)
    return lax.ppermute(value, axis, [(source, source ^ 1) for source in range(count)])


def split(value):
    high = value.astype(jnp.bfloat16)
    return high, (value - high.astype(jnp.float32)).astype(jnp.bfloat16)


def tables(side, half_rows):
    points = np.arange(side)
    angles = (points[:, None] * points[None, :] % side) * (2.0 * math.pi / side)
    hartley = (np.cos(angles) + np.sin(angles)).astype(np.float32)
    high = hartley.astype(jnp.bfloat16)
    low = (hartley - high.astype(np.float32)).astype(jnp.bfloat16)
    eye = np.eye(2, dtype=np.float32)
    wide_high = np.kron(eye, high.astype(np.float32))
    wide_low = np.kron(eye, low.astype(np.float32))
    right = np.block([[wide_high, wide_low], [wide_high, wide_low]]).astype(jnp.bfloat16)
    left = np.concatenate([high, high, low], 1)
    eigenvalues = 2.0 - 2.0 * np.cos(points * (2.0 * math.pi / side))
    shift = 1.0 / side**2 + eigenvalues[:, None] + np.tile(eigenvalues, 2)[None, :]
    ratio = 1.0 + shift / 2 - np.sqrt(shift + shift**2 / 4)
    power = ratio**half_rows
    reach = ratio**GROUP
    scale = 1.0 / side / (1.0 / ratio - ratio) / side**2
    wrap = 1.0 / (1.0 - power**4)
    decay = np.stack([ratio, power, scale, wrap, reach]).astype(np.float32)
    return right, left, decay


def along_last(value, right):
    width = value.shape[1]
    product = jnp.dot(
        jnp.concatenate(split(value), 1), right, preferred_element_type=jnp.float32
    )
    return product[:, :width] + product[:, width:]


def along_second(planes, left):
    width = planes[0].shape[1]
    out = []
    for start in range(0, len(planes), 2):
        both = jnp.concatenate(planes[start : start + 2], 1)
        high, low = split(both)
        stacked = jnp.concatenate([high, low, high], 0)
        product = jnp.dot(left, stacked, preferred_element_type=jnp.float32)
        out.append(product[:, :width])
        out.append(product[:, width:])
    return out


def halves(value):
    return pltpu.roll(value, value.shape[-1] // 2, axis=value.ndim - 1)


PARTS = 4
DIGIT = 3


def arrange_kernel(row, source, *refs):
    packed, raw, arrivals = refs[-3:]
    slab_rows, cells = raw.shape
    width = packed.shape[-1]
    half = slab_rows // 2
    lower = lax.broadcasted_iota(jnp.int32, (GROUP, width), 1) < width // 2
    tiles = 4
    parts = arrivals.shape[0]
    part = cells // parts
    copies = []
    for k in range(parts):
        lanes = pl.ds(k * part, part)
        copies.append(
            pltpu.make_async_copy(source.at[row, :, lanes], raw.at[:, lanes], arrivals.at[k])
        )
        copies[-1].start()

    def tile_step(step, carry):
        ys = pl.ds(pl.multiple_of(step * 2 * tiles, 2 * tiles), 2 * tiles)
        for start in range(0, half, GROUP):
            lines = []
            for k in range(tiles):
                lanes = pl.ds(pl.multiple_of((step * tiles + k) * width, width), width)
                near = raw[pl.ds(start, GROUP), lanes]
                far = raw[pl.ds(start + half, GROUP), lanes]
                lines.append(jnp.where(lower, near, halves(far)))
                lines.append(jnp.where(lower, halves(near), far))
            packed[pl.ds(start, GROUP), ys, :] = jnp.swapaxes(jnp.stack(lines, 0), 0, 1)
        return carry

    steps = part // (width * tiles)
    for k in range(parts):
        copies[k].wait()
        lax.fori_loop(k * steps, (k + 1) * steps, tile_step, 0)


def stack_kernel(first, second, own):
    own[0] = first[...]
    own[1] = second[...]


def restore_kernel(row, flag, own, passed, arrived, *refs):
    out = refs[-1]
    _, slab_rows, cells = out.shape
    width = own.shape[-1]
    half = slab_rows // 2
    lower = lax.broadcasted_iota(jnp.int32, (GROUP, width), 1) < width // 2
    weight = flag[0].astype(jnp.float32)
    tiles = 4

    steps = cells // (width * tiles)
    base = pl.program_id(0) * steps

    def tile_step(step, carry):
        ys = pl.ds(pl.multiple_of((base + step) * 2 * tiles, 2 * tiles), 2 * tiles)
        for start in range(0, half, GROUP):
            planes = pl.ds(start, GROUP)
            block = own[row, planes, ys, :] + weight * passed[planes, ys, :] + arrived[planes, ys, :]
            block = jnp.swapaxes(block, 0, 1)
            for k in range(tiles):
                lanes = pl.ds(pl.multiple_of((step * tiles + k) * width, width), width)
                even, odd = block[2 * k], block[2 * k + 1]
                out[0, planes, lanes] = jnp.where(lower, even, halves(odd))
                out[0, pl.ds(start + half, GROUP), lanes] = jnp.where(lower, halves(even), odd)
        return carry

    lax.fori_loop(0, steps, tile_step, 0)


def pick_kernel(flag, after, far, own, out):
    @pl.when(flag[0] == 0)
    def _():
        out[...] = far[...]

    @pl.when(flag[0] == 1)
    def _():
        out[...] = own[...]


def join_kernel(flag, after, distant, handed, out):
    weight = 1.0 - flag[0].astype(jnp.float32)
    out[...] = distant[...] + weight * handed[...]


def slab_moments(moments, i, reach):
    count = moments.shape[1]
    ahead = moments[i, 0, 0]
    behind = moments[i, count - 1, 1]
    for k in range(1, count):
        ahead = ahead * reach + moments[i, k, 0]
        behind = behind * reach + moments[i, count - 1 - k, 1]
    return ahead, behind


def forward_kernel(base, counts, after, own, other, right_ref, left_ref, decay, *refs):
    spectrum, moments, mine = refs[-3:]
    offset = mine.shape[0] - own.shape[0]
    if offset:
        mine[:offset] = refs[0][...]
    owned, rows, side, width = own.shape
    chunks = rows // GROUP
    lower = lax.broadcasted_iota(jnp.int32, (side, width), 1) < width // 2

    def orbital_step(i, carry):
        live = count_at(counts, base + i) > 0

        def chunk_step(c, carry):
            block = pl.ds(pl.multiple_of(c * GROUP, GROUP), GROUP)
            density = own[i, block] * other[block]
            value = along_last(density.reshape(GROUP * side, width), right_ref[...])
            planes = [value[k * side : (k + 1) * side] for k in range(GROUP)]
            planes = along_second(planes, left_ref[...])
            ratio = decay[0]
            ahead = planes[0]
            behind = planes[-1]
            for k in range(GROUP):
                spectrum[i, c * GROUP + k] = planes[k]
                if k:
                    ahead = ahead * ratio + planes[k]
                    behind = behind * ratio + planes[GROUP - 1 - k]
            moments[i, c, 0] = ahead
            moments[i, c, 1] = behind
            return carry

        lax.fori_loop(0, jnp.where(live, chunks, 0), chunk_step, 0)

        @pl.when(live)
        def _():
            power = decay[1]
            ahead, behind = slab_moments(moments, i, decay[4])
            mine[offset + i] = jnp.where(lower, behind + power * halves(behind), ahead + power * halves(ahead))

        return carry

    lax.fori_loop(0, owned, orbital_step, 0)


def backward_kernel(
    base, inside, offset, counts, after, own, other, spectrum, moments, mine, arrived,
    right_ref, left_ref, decay, *refs
):
    edge = refs[-1]
    if inside:
        before, total = refs[:2]
        total[...] = before[...]
    else:
        total, partner = refs[-3:-1]
        total[...] = refs[0][...] if len(refs) > 3 else jnp.zeros_like(total)
        partner[...] = jnp.zeros_like(partner)
    owned, rows, side, width = own.shape
    chunks = rows // GROUP
    lower = lax.broadcasted_iota(jnp.int32, (side, width), 1) < width // 2

    def orbital_step(i, carry):
        number = count_at(counts, base + i)

        @pl.when(number > 0)
        def _():
            power, reach = decay[1], decay[4]
            ahead_all, behind_all = slab_moments(moments, i, reach)
            entering = (arrived[offset + i] + power * power * mine[offset + i]) * decay[3]
            turned = halves(entering)
            ahead = jnp.where(lower, turned, halves(ahead_all) + power * entering)
            behind = jnp.where(lower, halves(behind_all) + power * entering, turned)
            edge[0, 0] = ahead
            edge[chunks - 1, 1] = behind
            for k in range(1, chunks):
                ahead = ahead * reach + moments[i, k - 1, 0]
                edge[k, 0] = ahead
                behind = behind * reach + moments[i, chunks - k, 1]
                edge[chunks - 1 - k, 1] = behind

        def chunk_step(c, carry):
            block = pl.ds(pl.multiple_of(c * GROUP, GROUP), GROUP)
            ratio = decay[0]
            scale = decay[2] * number.astype(jnp.float32)
            ahead = edge[c, 0]
            behind = edge[c, 1]
            tails = []
            for k in reversed(range(GROUP)):
                spilled = ratio * behind
                tails.insert(0, spilled)
                behind = spectrum[i, c * GROUP + k] + spilled
            planes = []
            for k in range(GROUP):
                ahead = spectrum[i, c * GROUP + k] + ratio * ahead
                planes.append(scale * (ahead + tails[k]))
            planes = along_second(planes, left_ref[...])
            value = along_last(jnp.concatenate(planes, 0), right_ref[...])
            potential = value.reshape(GROUP, side, width)
            total[i, block] += potential * other[block]
            if inside:
                total[1, block] += potential * own[i, block]
            else:
                partner[block] += potential * own[i, block]
            return carry

        lax.fori_loop(0, jnp.where(number > 0, chunks, 0), chunk_step, 0)
        return carry

    lax.fori_loop(0, owned, orbital_step, 0)


def pair_counts(pair_list, pair_count, owned, band_index, band_count):
    first, partner = pair_list[0, :, 0], pair_list[0, :, 1]
    live = jnp.arange(first.shape[0]) < pair_count[0]
    distance = (partner // owned - band_index) % band_count
    inside = (REACH * owned) * owned
    place = ((partner % owned) * REACH + distance - 1) * owned + first
    place = jnp.where(distance == 0, inside, place)
    return jnp.sum(jnp.where(live, lax.shift_left(1, DIGIT * place), 0)).reshape(1)


def count_at(counts, place):
    return lax.shift_right_logical(counts[0], DIGIT * place) & (2**DIGIT - 1)


def on_device(orbitals, pair_list, pair_count):
    owned, slab_rows, plane_cells = orbitals.shape
    side = math.isqrt(plane_cells)
    assert lax.axis_size("grid") == 2 and REACH == 2 and owned == 2
    rows = slab_rows // 2
    chunks = rows // GROUP
    band_count = lax.axis_size("band")
    band_index = lax.axis_index("band")
    right, left, decay = tables(side, rows)
    smem = pl.BlockSpec(memory_space=pltpu.SMEM)
    vmem = pl.BlockSpec(memory_space=pltpu.VMEM)
    free = pl.BlockSpec(memory_space=pl.ANY)
    hbm = pl.BlockSpec(memory_space=pltpu.HBM)
    params = pltpu.CompilerParams(vmem_limit_bytes=12 * 2**20)
    shape = (rows, side, 2 * side)
    one = jax.ShapeDtypeStruct(shape, jnp.float32)
    both = jax.ShapeDtypeStruct((owned,) + shape, jnp.float32)

    def call(kernel, out_shape, in_specs, out_specs=vmem, scratch=(), aliases={}, grid=()):
        if isinstance(out_shape, tuple):
            out_specs = (vmem,) * len(out_shape)
        return pl.pallas_call(
            kernel,
            out_shape=out_shape,
            grid=grid,
            in_specs=in_specs,
            out_specs=out_specs,
            scratch_shapes=scratch,
            compiler_params=params,
            input_output_aliases=aliases,
            cost_estimate=pl.CostEstimate(flops=0, bytes_accessed=1 << 20, transcendentals=0),
        )

    fields, far = [], []
    for row in range(owned):
        field = call(
            functools.partial(arrange_kernel, row),
            one,
            [hbm] + [free] * row,
            scratch=[
                pltpu.VMEM(orbitals.shape[1:], jnp.float32),
                pltpu.SemaphoreType.DMA((PARTS,)),
            ],
        )(orbitals, *fields)
        fields.append(field)
        far.append(rotated(field, "band", -2))
    own = call(stack_kernel, both, [vmem, vmem])(*fields)
    flag = (band_index % 2).reshape(1)
    counts = pair_counts(pair_list, pair_count, owned, band_index, band_count)

    def forward(base, after, other, *earlier):
        return call(
            functools.partial(forward_kernel, base),
            (
                both,
                jax.ShapeDtypeStruct((owned, chunks, 2) + shape[1:], jnp.float32),
                jax.ShapeDtypeStruct(((1 + len(earlier)) * owned,) + shape[1:], jnp.float32),
            ),
            [smem, free] + [vmem] * (5 + len(earlier)),
        )(counts, after, own, other, right, left, decay, *earlier)

    def exchanged(mine):
        return swapped(mine, "grid")

    def backward(base, after, state, total, inside=False, offset=0):
        return call(
            functools.partial(backward_kernel, base, inside, offset),
            both if inside else (both, one),
            [smem, free] + [vmem] * (9 + len(total)),
            scratch=[pltpu.VMEM((chunks, 2) + shape[1:], jnp.float32)],
        )(counts, after, own, *state, right, left, decay, *total)

    inner_base = REACH * owned * owned
    spectrum, moments, mine = forward(inner_base, own, fields[1])
    inner = (fields[1], spectrum, moments, mine, exchanged(mine))
    after = mine
    total, passed, arrived = (), [], []
    for row in range(owned):
        base = row * REACH * owned
        picked = call(pick_kernel, one, [smem, free, vmem, vmem])(
            flag, after, far[row], fields[row]
        )
        near = swapped(picked, "band")
        distant_state = forward(base + owned, picked, far[row])
        near_state = forward(base, distant_state[2], near, distant_state[2])
        mine = near_state[2]
        ends = (mine, exchanged(mine))
        near_state = (near,) + tuple(near_state[:2]) + ends
        distant_state = (far[row],) + tuple(distant_state[:2]) + ends
        acc, handed = backward(base, mine, near_state, total, offset=owned)
        handed_over = swapped(handed, "band")
        acc, distant = backward(base + owned, handed, distant_state, (acc,))
        total = (acc,)
        joined = call(join_kernel, one, [smem, free, vmem, vmem])(
            flag, distant, distant, handed_over
        )
        passed.append(handed_over)
        arrived.append(rotated(joined, "band", 2))
        after = joined
    total = backward(inner_base, after, inner, total, inside=True)
    out = jax.ShapeDtypeStruct(orbitals.shape, jnp.float32)
    result = None
    for row in range(owned):
        earlier = [] if result is None else [result]
        result = call(
            functools.partial(restore_kernel, row),
            out,
            [smem] + [vmem] * 3 + [free] * len(earlier),
            out_specs=pl.BlockSpec(
                (1, slab_rows, plane_cells // PARTS),
                functools.partial(lambda r, step: (r, 0, step), row),
            ),
            grid=(PARTS,),
            aliases={4: 0} if earlier else {},
        )(flag, total, passed[row], arrived[row], *earlier)
    return result


def solution(mesh):
    in_specs = (P("band", "grid", None), P("band", None, None), P("band"))
    out_specs = P("band", "grid", None)

    return jax.shard_map(
        on_device, mesh=mesh, in_specs=in_specs, out_specs=out_specs, check_vma=False
    )
```

```python
import functools
import math

import jax
import jax.numpy as jnp
import numpy as np
from jax import lax
from jax.experimental import pallas as pl
from jax.experimental.pallas import tpu as pltpu
from jax.sharding import PartitionSpec as P

REACH = 2
GROUP = 8


def rotated(value, axis, steps):
    count = lax.axis_size(axis)
    pairs = [(source, (source + steps) % count) for source in range(count)]
    return lax.ppermute(value, axis, pairs)


def swapped(value, axis):
    count = lax.axis_size(axis)
    return lax.ppermute(value, axis, [(source, source ^ 1) for source in range(count)])


def split(value):
    high = value.astype(jnp.bfloat16)
    return high, (value - high.astype(jnp.float32)).astype(jnp.bfloat16)


def tables(side, half_rows):
    points = np.arange(side)
    angles = (points[:, None] * points[None, :] % side) * (2.0 * math.pi / side)
    hartley = (np.cos(angles) + np.sin(angles)).astype(np.float32)
    high = hartley.astype(jnp.bfloat16)
    low = (hartley - high.astype(np.float32)).astype(jnp.bfloat16)
    eye = np.eye(2, dtype=np.float32)
    wide_high = np.kron(eye, high.astype(np.float32))
    wide_low = np.kron(eye, low.astype(np.float32))
    right = np.block([[wide_high, wide_low], [wide_high, wide_low]]).astype(jnp.bfloat16)
    left = np.concatenate([high, high, low], 1)
    eigenvalues = 2.0 - 2.0 * np.cos(points * (2.0 * math.pi / side))
    shift = 1.0 / side**2 + eigenvalues[:, None] + np.tile(eigenvalues, 2)[None, :]
    ratio = 1.0 + shift / 2 - np.sqrt(shift + shift**2 / 4)
    power = ratio**half_rows
    reach = ratio**GROUP
    scale = 1.0 / side / (1.0 / ratio - ratio) / side**2
    wrap = 1.0 / (1.0 - power**4)
    decay = np.stack([ratio, power, scale, wrap, reach]).astype(np.float32)
    return right, left, decay


def along_last(value, right):
    width = value.shape[1]
    product = jnp.dot(
        jnp.concatenate(split(value), 1), right, preferred_element_type=jnp.float32
    )
    return product[:, :width] + product[:, width:]


def along_second(planes, left):
    width = planes[0].shape[1]
    out = []
    for start in range(0, len(planes), 2):
        both = jnp.concatenate(planes[start : start + 2], 1)
        high, low = split(both)
        stacked = jnp.concatenate([high, low, high], 0)
        product = jnp.dot(left, stacked, preferred_element_type=jnp.float32)
        out.append(product[:, :width])
        out.append(product[:, width:])
    return out


def halves(value):
    return pltpu.roll(value, value.shape[-1] // 2, axis=value.ndim - 1)


PARTS = 4
DIGIT = 3


def arrange_kernel(row, source, *refs):
    packed, raw, arrivals = refs[-3:]
    slab_rows, cells = raw.shape
    width = packed.shape[-1]
    half = slab_rows // 2
    lower = lax.broadcasted_iota(jnp.int32, (GROUP, width), 1) < width // 2
    tiles = 4
    parts = arrivals.shape[0]
    part = cells // parts
    copies = []
    for k in range(parts):
        lanes = pl.ds(k * part, part)
        copies.append(
            pltpu.make_async_copy(source.at[row, :, lanes], raw.at[:, lanes], arrivals.at[k])
        )
        copies[-1].start()

    def tile_step(step, carry):
        ys = pl.ds(pl.multiple_of(step * 2 * tiles, 2 * tiles), 2 * tiles)
        for start in range(0, half, GROUP):
            lines = []
            for k in range(tiles):
                lanes = pl.ds(pl.multiple_of((step * tiles + k) * width, width), width)
                near = raw[pl.ds(start, GROUP), lanes]
                far = raw[pl.ds(start + half, GROUP), lanes]
                lines.append(jnp.where(lower, near, halves(far)))
                lines.append(jnp.where(lower, halves(near), far))
            packed[pl.ds(start, GROUP), ys, :] = jnp.swapaxes(jnp.stack(lines, 0), 0, 1)
        return carry

    steps = part // (width * tiles)
    for k in range(parts):
        copies[k].wait()
        lax.fori_loop(k * steps, (k + 1) * steps, tile_step, 0)


def stack_kernel(first, second, own):
    own[0] = first[...]
    own[1] = second[...]


def restore_kernel(row, flag, own, passed, arrived, *refs):
    out, raw, departures = refs[-3:]
    slab_rows, cells = raw.shape
    width = own.shape[-1]
    half = slab_rows // 2
    lower = lax.broadcasted_iota(jnp.int32, (GROUP, width), 1) < width // 2
    weight = flag[0].astype(jnp.float32)
    tiles = 4
    parts = departures.shape[0]
    part = cells // parts

    def tile_step(step, carry):
        ys = pl.ds(pl.multiple_of(step * 2 * tiles, 2 * tiles), 2 * tiles)
        for start in range(0, half, GROUP):
            planes = pl.ds(start, GROUP)
            block = own[row, planes, ys, :] + weight * passed[planes, ys, :] + arrived[planes, ys, :]
            block = jnp.swapaxes(block, 0, 1)
            for k in range(tiles):
                lanes = pl.ds(pl.multiple_of((step * tiles + k) * width, width), width)
                even, odd = block[2 * k], block[2 * k + 1]
                raw[planes, lanes] = jnp.where(lower, even, halves(odd))
                raw[pl.ds(start + half, GROUP), lanes] = jnp.where(lower, halves(even), odd)
        return carry

    steps = part // (width * tiles)
    copies = []
    for k in range(parts):
        lax.fori_loop(k * steps, (k + 1) * steps, tile_step, 0)
        lanes = pl.ds(k * part, part)
        copies.append(
            pltpu.make_async_copy(raw.at[:, lanes], out.at[row, :, lanes], departures.at[k])
        )
        copies[-1].start()
    for copy in copies:
        copy.wait()


def pick_kernel(flag, after, far, own, out):
    @pl.when(flag[0] == 0)
    def _():
        out[...] = far[...]

    @pl.when(flag[0] == 1)
    def _():
        out[...] = own[...]


def join_kernel(flag, after, distant, handed, out):
    weight = 1.0 - flag[0].astype(jnp.float32)
    out[...] = distant[...] + weight * handed[...]


def slab_moments(moments, i, reach):
    count = moments.shape[1]
    ahead = moments[i, 0, 0]
    behind = moments[i, count - 1, 1]
    for k in range(1, count):
        ahead = ahead * reach + moments[i, k, 0]
        behind = behind * reach + moments[i, count - 1 - k, 1]
    return ahead, behind


def forward_kernel(base, counts, after, own, other, right_ref, left_ref, decay, *refs):
    spectrum, moments, mine = refs[-3:]
    offset = mine.shape[0] - own.shape[0]
    if offset:
        mine[:offset] = refs[0][...]
    owned, rows, side, width = own.shape
    chunks = rows // GROUP
    lower = lax.broadcasted_iota(jnp.int32, (side, width), 1) < width // 2

    def orbital_step(i, carry):
        live = count_at(counts, base + i) > 0

        def chunk_step(c, carry):
            block = pl.ds(pl.multiple_of(c * GROUP, GROUP), GROUP)
            density = own[i, block] * other[block]
            value = along_last(density.reshape(GROUP * side, width), right_ref[...])
            planes = [value[k * side : (k + 1) * side] for k in range(GROUP)]
            planes = along_second(planes, left_ref[...])
            ratio = decay[0]
            ahead = planes[0]
            behind = planes[-1]
            for k in range(GROUP):
                spectrum[i, c * GROUP + k] = planes[k]
                if k:
                    ahead = ahead * ratio + planes[k]
                    behind = behind * ratio + planes[GROUP - 1 - k]
            moments[i, c, 0] = ahead
            moments[i, c, 1] = behind
            return carry

        lax.fori_loop(0, jnp.where(live, chunks, 0), chunk_step, 0)

        @pl.when(live)
        def _():
            power = decay[1]
            ahead, behind = slab_moments(moments, i, decay[4])
            mine[offset + i] = jnp.where(lower, behind + power * halves(behind), ahead + power * halves(ahead))

        return carry

    lax.fori_loop(0, owned, orbital_step, 0)


def backward_kernel(
    base, inside, offset, counts, after, own, other, spectrum, moments, mine, arrived,
    right_ref, left_ref, decay, *refs
):
    edge = refs[-1]
    if inside:
        before, total = refs[:2]
        total[...] = before[...]
    else:
        total, partner = refs[-3:-1]
        total[...] = refs[0][...] if len(refs) > 3 else jnp.zeros_like(total)
        partner[...] = jnp.zeros_like(partner)
    owned, rows, side, width = own.shape
    chunks = rows // GROUP
    lower = lax.broadcasted_iota(jnp.int32, (side, width), 1) < width // 2

    def orbital_step(i, carry):
        number = count_at(counts, base + i)

        @pl.when(number > 0)
        def _():
            power, reach = decay[1], decay[4]
            ahead_all, behind_all = slab_moments(moments, i, reach)
            entering = (arrived[offset + i] + power * power * mine[offset + i]) * decay[3]
            turned = halves(entering)
            ahead = jnp.where(lower, turned, halves(ahead_all) + power * entering)
            behind = jnp.where(lower, halves(behind_all) + power * entering, turned)
            edge[0, 0] = ahead
            edge[chunks - 1, 1] = behind
            for k in range(1, chunks):
                ahead = ahead * reach + moments[i, k - 1, 0]
                edge[k, 0] = ahead
                behind = behind * reach + moments[i, chunks - k, 1]
                edge[chunks - 1 - k, 1] = behind

        def chunk_step(c, carry):
            block = pl.ds(pl.multiple_of(c * GROUP, GROUP), GROUP)
            ratio = decay[0]
            scale = decay[2] * number.astype(jnp.float32)
            ahead = edge[c, 0]
            behind = edge[c, 1]
            tails = []
            for k in reversed(range(GROUP)):
                spilled = ratio * behind
                tails.insert(0, spilled)
                behind = spectrum[i, c * GROUP + k] + spilled
            planes = []
            for k in range(GROUP):
                ahead = spectrum[i, c * GROUP + k] + ratio * ahead
                planes.append(scale * (ahead + tails[k]))
            planes = along_second(planes, left_ref[...])
            value = along_last(jnp.concatenate(planes, 0), right_ref[...])
            potential = value.reshape(GROUP, side, width)
            total[i, block] += potential * other[block]
            if inside:
                total[1, block] += potential * own[i, block]
            else:
                partner[block] += potential * own[i, block]
            return carry

        lax.fori_loop(0, jnp.where(number > 0, chunks, 0), chunk_step, 0)
        return carry

    lax.fori_loop(0, owned, orbital_step, 0)


def pair_counts(pair_list, pair_count, owned, band_index, band_count):
    first, partner = pair_list[0, :, 0], pair_list[0, :, 1]
    live = jnp.arange(first.shape[0]) < pair_count[0]
    distance = (partner // owned - band_index) % band_count
    inside = (REACH * owned) * owned
    place = ((partner % owned) * REACH + distance - 1) * owned + first
    place = jnp.where(distance == 0, inside, place)
    return jnp.sum(jnp.where(live, lax.shift_left(1, DIGIT * place), 0)).reshape(1)


def count_at(counts, place):
    return lax.shift_right_logical(counts[0], DIGIT * place) & (2**DIGIT - 1)


def on_device(orbitals, pair_list, pair_count):
    owned, slab_rows, plane_cells = orbitals.shape
    side = math.isqrt(plane_cells)
    assert lax.axis_size("grid") == 2 and REACH == 2 and owned == 2
    rows = slab_rows // 2
    chunks = rows // GROUP
    band_count = lax.axis_size("band")
    band_index = lax.axis_index("band")
    right, left, decay = tables(side, rows)
    smem = pl.BlockSpec(memory_space=pltpu.SMEM)
    vmem = pl.BlockSpec(memory_space=pltpu.VMEM)
    free = pl.BlockSpec(memory_space=pl.ANY)
    hbm = pl.BlockSpec(memory_space=pltpu.HBM)
    params = pltpu.CompilerParams(vmem_limit_bytes=12 * 2**20)
    shape = (rows, side, 2 * side)
    one = jax.ShapeDtypeStruct(shape, jnp.float32)
    both = jax.ShapeDtypeStruct((owned,) + shape, jnp.float32)

    def call(kernel, out_shape, in_specs, out_specs=vmem, scratch=(), aliases={}):
        if isinstance(out_shape, tuple):
            out_specs = (vmem,) * len(out_shape)
        return pl.pallas_call(
            kernel,
            out_shape=out_shape,
            in_specs=in_specs,
            out_specs=out_specs,
            scratch_shapes=scratch,
            compiler_params=params,
            input_output_aliases=aliases,
            cost_estimate=pl.CostEstimate(flops=0, bytes_accessed=1 << 20, transcendentals=0),
        )

    source = pltpu.with_memory_space_constraint(orbitals, pltpu.HBM)
    fields, far = [], []
    for row in range(owned):
        field = call(
            functools.partial(arrange_kernel, row),
            one,
            [hbm] + [free] * row,
            scratch=[
                pltpu.VMEM(orbitals.shape[1:], jnp.float32),
                pltpu.SemaphoreType.DMA((PARTS,)),
            ],
        )(source, *fields)
        fields.append(field)
        far.append(rotated(field, "band", -2))
    own = call(stack_kernel, both, [vmem, vmem])(*fields)
    flag = (band_index % 2).reshape(1)
    counts = pair_counts(pair_list, pair_count, owned, band_index, band_count)

    def forward(base, after, other, *earlier):
        return call(
            functools.partial(forward_kernel, base),
            (
                both,
                jax.ShapeDtypeStruct((owned, chunks, 2) + shape[1:], jnp.float32),
                jax.ShapeDtypeStruct(((1 + len(earlier)) * owned,) + shape[1:], jnp.float32),
            ),
            [smem, free] + [vmem] * (5 + len(earlier)),
        )(counts, after, own, other, right, left, decay, *earlier)

    def exchanged(mine):
        return swapped(mine, "grid")

    def backward(base, after, state, total, inside=False, offset=0):
        return call(
            functools.partial(backward_kernel, base, inside, offset),
            both if inside else (both, one),
            [smem, free] + [vmem] * (9 + len(total)),
            scratch=[pltpu.VMEM((chunks, 2) + shape[1:], jnp.float32)],
        )(counts, after, own, *state, right, left, decay, *total)

    inner_base = REACH * owned * owned
    spectrum, moments, mine = forward(inner_base, own, fields[1])
    inner = (fields[1], spectrum, moments, mine, exchanged(mine))
    after = mine

    def brought(row, after):
        picked = call(pick_kernel, one, [smem, free, vmem, vmem])(
            flag, after, far[row], fields[row]
        )
        return picked, swapped(picked, "band")

    total, passed, arrived = (), [], []
    after, near = brought(0, after)
    for row in range(owned):
        base = row * REACH * owned
        distant_state = forward(base + owned, after, far[row])
        near_state = forward(base, distant_state[2], near, distant_state[2])
        mine = near_state[2]
        ends = (mine, exchanged(mine))
        near_state = (near,) + tuple(near_state[:2]) + ends
        distant_state = (far[row],) + tuple(distant_state[:2]) + ends
        acc, handed = backward(base, mine, near_state, total, offset=owned)
        handed_over = swapped(handed, "band")
        after = handed
        if row + 1 < owned:
            after, near = brought(row + 1, handed)
        acc, distant = backward(base + owned, after, distant_state, (acc,))
        total = (acc,)
        joined = call(join_kernel, one, [smem, free, vmem, vmem])(
            flag, distant, distant, handed_over
        )
        passed.append(handed_over)
        arrived.append(rotated(joined, "band", 2))
        after = joined
    total = backward(inner_base, after, inner, total, inside=True)
    out = jax.ShapeDtypeStruct(orbitals.shape, jnp.float32)
    result = None
    for row in range(owned):
        earlier = [] if result is None else [result]
        result = call(
            functools.partial(restore_kernel, row),
            out,
            [smem] + [vmem] * 3 + [hbm] * len(earlier),
            out_specs=hbm,
            scratch=[
                pltpu.VMEM(orbitals.shape[1:], jnp.float32),
                pltpu.SemaphoreType.DMA((PARTS,)),
            ],
            aliases={4: 0} if earlier else {},
        )(flag, total, passed[row], arrived[row], *earlier)
    return result


def solution(mesh):
    in_specs = (P("band", "grid", None), P("band", None, None), P("band"))
    out_specs = P("band", "grid", None)

    return jax.shard_map(
        on_device, mesh=mesh, in_specs=in_specs, out_specs=out_specs, check_vma=False
    )
```

```python
import functools
import math

import jax
import jax.numpy as jnp
import numpy as np
from jax import lax
from jax.experimental import pallas as pl
from jax.experimental.pallas import tpu as pltpu
from jax.sharding import PartitionSpec as P

REACH = 2
GROUP = 8


def rotated(value, axis, steps):
    count = lax.axis_size(axis)
    pairs = [(source, (source + steps) % count) for source in range(count)]
    return lax.ppermute(value, axis, pairs)


def swapped(value, axis):
    count = lax.axis_size(axis)
    return lax.ppermute(value, axis, [(source, source ^ 1) for source in range(count)])


def split(value):
    high = value.astype(jnp.bfloat16)
    return high, (value - high.astype(jnp.float32)).astype(jnp.bfloat16)


def tables(side, half_rows):
    points = np.arange(side)
    angles = (points[:, None] * points[None, :] % side) * (2.0 * math.pi / side)
    hartley = (np.cos(angles) + np.sin(angles)).astype(np.float32)
    high = hartley.astype(jnp.bfloat16)
    low = (hartley - high.astype(np.float32)).astype(jnp.bfloat16)
    eye = np.eye(2, dtype=np.float32)
    wide_high = np.kron(eye, high.astype(np.float32))
    wide_low = np.kron(eye, low.astype(np.float32))
    right = np.block([[wide_high, wide_low], [wide_high, wide_low]]).astype(jnp.bfloat16)
    left = np.concatenate([high, high, low], 1)
    eigenvalues = 2.0 - 2.0 * np.cos(points * (2.0 * math.pi / side))
    shift = 1.0 / side**2 + eigenvalues[:, None] + np.tile(eigenvalues, 2)[None, :]
    ratio = 1.0 + shift / 2 - np.sqrt(shift + shift**2 / 4)
    power = ratio**half_rows
    reach = ratio**GROUP
    scale = 1.0 / side / (1.0 / ratio - ratio) / side**2
    wrap = 1.0 / (1.0 - power**4)
    decay = np.stack([ratio, power, scale, wrap, reach]).astype(np.float32)
    return right, left, decay


def along_last(value, right):
    width = value.shape[1]
    product = jnp.dot(
        jnp.concatenate(split(value), 1), right, preferred_element_type=jnp.float32
    )
    return product[:, :width] + product[:, width:]


def along_second(planes, left):
    width = planes[0].shape[1]
    out = []
    for start in range(0, len(planes), 2):
        both = jnp.concatenate(planes[start : start + 2], 1)
        high, low = split(both)
        stacked = jnp.concatenate([high, low, high], 0)
        product = jnp.dot(left, stacked, preferred_element_type=jnp.float32)
        out.append(product[:, :width])
        out.append(product[:, width:])
    return out


def halves(value):
    return pltpu.roll(value, value.shape[-1] // 2, axis=value.ndim - 1)


PARTS = 4
DIGIT = 3


def arrange_kernel(row, source, *refs):
    packed, raw, arrivals = refs[-3:]
    slab_rows, cells = raw.shape
    width = packed.shape[-1]
    half = slab_rows // 2
    lower = lax.broadcasted_iota(jnp.int32, (GROUP, width), 1) < width // 2
    tiles = 4
    parts = arrivals.shape[0]
    part = cells // parts
    copies = []
    for k in range(parts):
        lanes = pl.ds(k * part, part)
        copies.append(
            pltpu.make_async_copy(source.at[row, :, lanes], raw.at[:, lanes], arrivals.at[k])
        )
        copies[-1].start()

    def tile_step(step, carry):
        ys = pl.ds(pl.multiple_of(step * 2 * tiles, 2 * tiles), 2 * tiles)
        for start in range(0, half, GROUP):
            lines = []
            for k in range(tiles):
                lanes = pl.ds(pl.multiple_of((step * tiles + k) * width, width), width)
                near = raw[pl.ds(start, GROUP), lanes]
                far = raw[pl.ds(start + half, GROUP), lanes]
                lines.append(jnp.where(lower, near, halves(far)))
                lines.append(jnp.where(lower, halves(near), far))
            packed[pl.ds(start, GROUP), ys, :] = jnp.swapaxes(jnp.stack(lines, 0), 0, 1)
        return carry

    steps = part // (width * tiles)
    for k in range(parts):
        copies[k].wait()
        lax.fori_loop(k * steps, (k + 1) * steps, tile_step, 0)


def stack_kernel(first, second, own):
    own[0] = first[...]
    own[1] = second[...]


def restore_kernel(row, flag, own, passed, arrived, *refs):
    out, raw, departures = refs[-3:]
    slab_rows, cells = raw.shape
    width = own.shape[-1]
    half = slab_rows // 2
    lower = lax.broadcasted_iota(jnp.int32, (GROUP, width), 1) < width // 2
    weight = flag[0].astype(jnp.float32)
    tiles = 4
    parts = departures.shape[0]
    part = cells // parts

    def tile_step(step, carry):
        ys = pl.ds(pl.multiple_of(step * 2 * tiles, 2 * tiles), 2 * tiles)
        for start in range(0, half, GROUP):
            planes = pl.ds(start, GROUP)
            block = own[row, planes, ys, :] + weight * passed[planes, ys, :] + arrived[planes, ys, :]
            block = jnp.swapaxes(block, 0, 1)
            for k in range(tiles):
                lanes = pl.ds(pl.multiple_of((step * tiles + k) * width, width), width)
                even, odd = block[2 * k], block[2 * k + 1]
                raw[planes, lanes] = jnp.where(lower, even, halves(odd))
                raw[pl.ds(start + half, GROUP), lanes] = jnp.where(lower, halves(even), odd)
        return carry

    steps = part // (width * tiles)
    copies = []
    for k in range(parts):
        lax.fori_loop(k * steps, (k + 1) * steps, tile_step, 0)
        lanes = pl.ds(k * part, part)
        copies.append(
            pltpu.make_async_copy(raw.at[:, lanes], out.at[row, :, lanes], departures.at[k])
        )
        copies[-1].start()
    for copy in copies:
        copy.wait()


def pick_kernel(flag, after, far, own, out):
    @pl.when(flag[0] == 0)
    def _():
        out[...] = far[...]

    @pl.when(flag[0] == 1)
    def _():
        out[...] = own[...]


def join_kernel(flag, after, distant, handed, out):
    weight = 1.0 - flag[0].astype(jnp.float32)
    out[...] = distant[...] + weight * handed[...]


def slab_moments(moments, i, reach):
    count = moments.shape[1]
    ahead = moments[i, 0, 0]
    behind = moments[i, count - 1, 1]
    for k in range(1, count):
        ahead = ahead * reach + moments[i, k, 0]
        behind = behind * reach + moments[i, count - 1 - k, 1]
    return ahead, behind


def forward_kernel(base, counts, after, own, other, right_ref, left_ref, decay, *refs):
    spectrum, moments, mine = refs
    owned, rows, side, width = own.shape
    chunks = rows // GROUP
    lower = lax.broadcasted_iota(jnp.int32, (side, width), 1) < width // 2

    def orbital_step(i, carry):
        live = count_at(counts, base + i) > 0

        def chunk_step(c, carry):
            block = pl.ds(pl.multiple_of(c * GROUP, GROUP), GROUP)
            density = own[i, block] * other[block]
            value = along_last(density.reshape(GROUP * side, width), right_ref[...])
            planes = [value[k * side : (k + 1) * side] for k in range(GROUP)]
            planes = along_second(planes, left_ref[...])
            ratio = decay[0]
            ahead = planes[0]
            behind = planes[-1]
            for k in range(GROUP):
                spectrum[i, c * GROUP + k] = planes[k]
                if k:
                    ahead = ahead * ratio + planes[k]
                    behind = behind * ratio + planes[GROUP - 1 - k]
            moments[i, c, 0] = ahead
            moments[i, c, 1] = behind
            return carry

        lax.fori_loop(0, jnp.where(live, chunks, 0), chunk_step, 0)

        @pl.when(live)
        def _():
            power = decay[1]
            ahead, behind = slab_moments(moments, i, decay[4])
            mine[i] = jnp.where(lower, behind + power * halves(behind), ahead + power * halves(ahead))

        return carry

    lax.fori_loop(0, owned, orbital_step, 0)


def backward_kernel(
    base, inside, counts, after, own, other, spectrum, moments, mine, arrived,
    right_ref, left_ref, decay, *refs
):
    edge = refs[-1]
    if inside:
        before, total = refs[:2]
        total[...] = before[...]
    else:
        total, partner = refs[-3:-1]
        total[...] = refs[0][...] if len(refs) > 3 else jnp.zeros_like(total)
        partner[...] = jnp.zeros_like(partner)
    owned, rows, side, width = own.shape
    chunks = rows // GROUP
    lower = lax.broadcasted_iota(jnp.int32, (side, width), 1) < width // 2

    def orbital_step(i, carry):
        number = count_at(counts, base + i)

        @pl.when(number > 0)
        def _():
            power, reach = decay[1], decay[4]
            ahead_all, behind_all = slab_moments(moments, i, reach)
            entering = (arrived[i] + power * power * mine[i]) * decay[3]
            turned = halves(entering)
            ahead = jnp.where(lower, turned, halves(ahead_all) + power * entering)
            behind = jnp.where(lower, halves(behind_all) + power * entering, turned)
            edge[0, 0] = ahead
            edge[chunks - 1, 1] = behind
            for k in range(1, chunks):
                ahead = ahead * reach + moments[i, k - 1, 0]
                edge[k, 0] = ahead
                behind = behind * reach + moments[i, chunks - k, 1]
                edge[chunks - 1 - k, 1] = behind

        def chunk_step(c, carry):
            block = pl.ds(pl.multiple_of(c * GROUP, GROUP), GROUP)
            ratio = decay[0]
            scale = decay[2] * number.astype(jnp.float32)
            ahead = edge[c, 0]
            behind = edge[c, 1]
            tails = []
            for k in reversed(range(GROUP)):
                spilled = ratio * behind
                tails.insert(0, spilled)
                behind = spectrum[i, c * GROUP + k] + spilled
            planes = []
            for k in range(GROUP):
                ahead = spectrum[i, c * GROUP + k] + ratio * ahead
                planes.append(scale * (ahead + tails[k]))
            planes = along_second(planes, left_ref[...])
            value = along_last(jnp.concatenate(planes, 0), right_ref[...])
            potential = value.reshape(GROUP, side, width)
            total[i, block] += potential * other[block]
            if inside:
                total[1, block] += potential * own[i, block]
            else:
                partner[block] += potential * own[i, block]
            return carry

        lax.fori_loop(0, jnp.where(number > 0, chunks, 0), chunk_step, 0)
        return carry

    lax.fori_loop(0, owned, orbital_step, 0)


def pair_counts(pair_list, pair_count, owned, band_index, band_count):
    first, partner = pair_list[0, :, 0], pair_list[0, :, 1]
    live = jnp.arange(first.shape[0]) < pair_count[0]
    distance = (partner // owned - band_index) % band_count
    inside = (REACH * owned) * owned
    place = ((partner % owned) * REACH + distance - 1) * owned + first
    place = jnp.where(distance == 0, inside, place)
    return jnp.sum(jnp.where(live, lax.shift_left(1, DIGIT * place), 0))


def count_at(counts, place):
    return lax.shift_right_logical(counts[0], 1 + DIGIT * place) & (2**DIGIT - 1)


def on_device(orbitals, pair_list, pair_count):
    owned, slab_rows, plane_cells = orbitals.shape
    side = math.isqrt(plane_cells)
    assert lax.axis_size("grid") == 2 and REACH == 2 and owned == 2
    rows = slab_rows // 2
    chunks = rows // GROUP
    band_count = lax.axis_size("band")
    band_index = lax.axis_index("band")
    right, left, decay = tables(side, rows)
    smem = pl.BlockSpec(memory_space=pltpu.SMEM)
    vmem = pl.BlockSpec(memory_space=pltpu.VMEM)
    free = pl.BlockSpec(memory_space=pl.ANY)
    hbm = pl.BlockSpec(memory_space=pltpu.HBM)
    params = pltpu.CompilerParams(vmem_limit_bytes=12 * 2**20)
    shape = (rows, side, 2 * side)
    one = jax.ShapeDtypeStruct(shape, jnp.float32)
    both = jax.ShapeDtypeStruct((owned,) + shape, jnp.float32)

    def call(kernel, out_shape, in_specs, out_specs=vmem, scratch=(), aliases={}):
        if isinstance(out_shape, tuple):
            out_specs = (vmem,) * len(out_shape)
        return pl.pallas_call(
            kernel,
            out_shape=out_shape,
            in_specs=in_specs,
            out_specs=out_specs,
            scratch_shapes=scratch,
            compiler_params=params,
            input_output_aliases=aliases,
            cost_estimate=pl.CostEstimate(flops=0, bytes_accessed=1 << 20, transcendentals=0),
        )

    source = pltpu.with_memory_space_constraint(orbitals, pltpu.HBM)
    fields, far = [], []
    for row in range(owned):
        field = call(
            functools.partial(arrange_kernel, row),
            one,
            [hbm] + [free] * row,
            scratch=[
                pltpu.VMEM(orbitals.shape[1:], jnp.float32),
                pltpu.SemaphoreType.DMA((PARTS,)),
            ],
        )(source, *fields)
        fields.append(field)
        far.append(rotated(field, "band", -2))
    own = call(stack_kernel, both, [vmem, vmem])(*fields)
    flag = (band_index % 2).reshape(1)
    counts = pair_counts(pair_list, pair_count, owned, band_index, band_count)
    counts = (lax.optimization_barrier(counts) * 2 + band_index % 2).reshape(1)

    def forward(base, after, other):
        return call(
            functools.partial(forward_kernel, base),
            (
                both,
                jax.ShapeDtypeStruct((owned, chunks, 2) + shape[1:], jnp.float32),
                jax.ShapeDtypeStruct((owned,) + shape[1:], jnp.float32),
            ),
            [smem, free] + [vmem] * 5,
        )(counts, after, own, other, right, left, decay)

    def exchanged(mine):
        return swapped(mine, "grid")

    def backward(base, after, state, total, inside=False):
        return call(
            functools.partial(backward_kernel, base, inside),
            both if inside else (both, one),
            [smem, free] + [vmem] * (9 + len(total)),
            scratch=[pltpu.VMEM((chunks, 2) + shape[1:], jnp.float32)],
        )(counts, after, own, *state, right, left, decay, *total)

    inner_base = REACH * owned * owned
    spectrum, moments, mine = forward(inner_base, own, fields[1])
    inner = (fields[1], spectrum, moments, mine, exchanged(mine))
    after = mine

    def brought(row, after):
        picked = call(pick_kernel, one, [smem, free, vmem, vmem])(
            flag, after, far[row], fields[row]
        )
        return picked, swapped(picked, "band")

    total, passed, arrived = (), [], []
    after, near = brought(0, after)
    for row in range(owned):
        base = row * REACH * owned
        distant_state = forward(base + owned, after, far[row])
        distant_ends = exchanged(distant_state[2])
        near_state = forward(base, distant_state[2], near)
        mine = near_state[2]
        near_state = (near,) + tuple(near_state) + (exchanged(mine),)
        distant_state = (far[row],) + tuple(distant_state) + (distant_ends,)
        acc, handed = backward(base, mine, near_state, total)
        handed_over = swapped(handed, "band")
        after = handed
        if row + 1 < owned:
            after, near = brought(row + 1, handed)
        acc, distant = backward(base + owned, after, distant_state, (acc,))
        total = (acc,)
        joined = call(join_kernel, one, [smem, free, vmem, vmem])(
            flag, distant, distant, handed_over
        )
        passed.append(handed_over)
        arrived.append(rotated(joined, "band", 2))
        after = joined
    total = backward(inner_base, after, inner, total, inside=True)
    out = jax.ShapeDtypeStruct(orbitals.shape, jnp.float32)
    result = None
    for row in range(owned):
        earlier = [] if result is None else [result]
        result = call(
            functools.partial(restore_kernel, row),
            out,
            [smem] + [vmem] * 3 + [hbm] * len(earlier),
            out_specs=hbm,
            scratch=[
                pltpu.VMEM(orbitals.shape[1:], jnp.float32),
                pltpu.SemaphoreType.DMA((PARTS,)),
            ],
            aliases={4: 0} if earlier else {},
        )(flag, total, passed[row], arrived[row], *earlier)
    return result


def solution(mesh):
    in_specs = (P("band", "grid", None), P("band", None, None), P("band"))
    out_specs = P("band", "grid", None)

    return jax.shard_map(
        on_device, mesh=mesh, in_specs=in_specs, out_specs=out_specs, check_vma=False
    )
```

```python
import functools
import math

import jax
import jax.numpy as jnp
import numpy as np
from jax import lax
from jax.experimental import pallas as pl
from jax.experimental.pallas import tpu as pltpu
from jax.sharding import PartitionSpec as P

REACH = 2
GROUP = 8


def rotated(value, axis, steps):
    count = lax.axis_size(axis)
    pairs = [(source, (source + steps) % count) for source in range(count)]
    return lax.ppermute(value, axis, pairs)


def swapped(value, axis):
    count = lax.axis_size(axis)
    return lax.ppermute(value, axis, [(source, source ^ 1) for source in range(count)])


def split(value):
    high = value.astype(jnp.bfloat16)
    return high, (value - high.astype(jnp.float32)).astype(jnp.bfloat16)


def tables(side, half_rows):
    points = np.arange(side)
    angles = (points[:, None] * points[None, :] % side) * (2.0 * math.pi / side)
    hartley = (np.cos(angles) + np.sin(angles)).astype(np.float32)
    high = hartley.astype(jnp.bfloat16)
    low = (hartley - high.astype(np.float32)).astype(jnp.bfloat16)
    eye = np.eye(2, dtype=np.float32)
    wide_high = np.kron(eye, high.astype(np.float32))
    wide_low = np.kron(eye, low.astype(np.float32))
    right = np.block([[wide_high, wide_low], [wide_high, wide_low]]).astype(jnp.bfloat16)
    left = np.concatenate([high, high, low], 1)
    eigenvalues = 2.0 - 2.0 * np.cos(points * (2.0 * math.pi / side))
    shift = 1.0 / side**2 + eigenvalues[:, None] + np.tile(eigenvalues, 2)[None, :]
    ratio = 1.0 + shift / 2 - np.sqrt(shift + shift**2 / 4)
    power = ratio**half_rows
    reach = ratio**GROUP
    scale = 1.0 / side / (1.0 / ratio - ratio) / side**2
    wrap = 1.0 / (1.0 - power**4)
    decay = np.stack([ratio, power, scale, wrap, reach]).astype(np.float32)
    return right, left, decay


def along_last(value, right):
    width = value.shape[1]
    product = jnp.dot(
        jnp.concatenate(split(value), 1), right, preferred_element_type=jnp.float32
    )
    return product[:, :width] + product[:, width:]


def along_second(planes, left):
    width = planes[0].shape[1]
    out = []
    for start in range(0, len(planes), 2):
        both = jnp.concatenate(planes[start : start + 2], 1)
        high, low = split(both)
        stacked = jnp.concatenate([high, low, high], 0)
        product = jnp.dot(left, stacked, preferred_element_type=jnp.float32)
        out.append(product[:, :width])
        out.append(product[:, width:])
    return out


def halves(value):
    return pltpu.roll(value, value.shape[-1] // 2, axis=value.ndim - 1)


PARTS = 4
DIGIT = 3


def arrange_kernel(row, source, *refs):
    packed, raw, arrivals = refs[-3:]
    slab_rows, cells = raw.shape
    width = packed.shape[-1]
    half = slab_rows // 2
    lower = lax.broadcasted_iota(jnp.int32, (GROUP, width), 1) < width // 2
    tiles = 4
    parts = arrivals.shape[0]
    part = cells // parts
    copies = []
    for k in range(parts):
        lanes = pl.ds(k * part, part)
        copies.append(
            pltpu.make_async_copy(source.at[row, :, lanes], raw.at[:, lanes], arrivals.at[k])
        )
        copies[-1].start()

    def tile_step(step, carry):
        ys = pl.ds(pl.multiple_of(step * 2 * tiles, 2 * tiles), 2 * tiles)
        for start in range(0, half, GROUP):
            lines = []
            for k in range(tiles):
                lanes = pl.ds(pl.multiple_of((step * tiles + k) * width, width), width)
                near = raw[pl.ds(start, GROUP), lanes]
                far = raw[pl.ds(start + half, GROUP), lanes]
                lines.append(jnp.where(lower, near, halves(far)))
                lines.append(jnp.where(lower, halves(near), far))
            packed[pl.ds(start, GROUP), ys, :] = jnp.swapaxes(jnp.stack(lines, 0), 0, 1)
        return carry

    steps = part // (width * tiles)
    for k in range(parts):
        copies[k].wait()
        lax.fori_loop(k * steps, (k + 1) * steps, tile_step, 0)


def stack_kernel(first, second, own):
    own[0] = first[...]
    own[1] = second[...]


def restore_kernel(row, flag, own, passed, arrived, *refs):
    out, raw, departures = refs[-3:]
    slab_rows, cells = raw.shape
    width = own.shape[-1]
    half = slab_rows // 2
    lower = lax.broadcasted_iota(jnp.int32, (GROUP, width), 1) < width // 2
    weight = flag[0].astype(jnp.float32)
    tiles = 4
    parts = departures.shape[0]
    part = cells // parts

    def tile_step(step, carry):
        ys = pl.ds(pl.multiple_of(step * 2 * tiles, 2 * tiles), 2 * tiles)
        for start in range(0, half, GROUP):
            planes = pl.ds(start, GROUP)
            block = own[row, planes, ys, :] + weight * passed[planes, ys, :] + arrived[planes, ys, :]
            block = jnp.swapaxes(block, 0, 1)
            for k in range(tiles):
                lanes = pl.ds(pl.multiple_of((step * tiles + k) * width, width), width)
                even, odd = block[2 * k], block[2 * k + 1]
                raw[planes, lanes] = jnp.where(lower, even, halves(odd))
                raw[pl.ds(start + half, GROUP), lanes] = jnp.where(lower, halves(even), odd)
        return carry

    steps = part // (width * tiles)
    copies = []
    for k in range(parts):
        lax.fori_loop(k * steps, (k + 1) * steps, tile_step, 0)
        lanes = pl.ds(k * part, part)
        copies.append(
            pltpu.make_async_copy(raw.at[:, lanes], out.at[row, :, lanes], departures.at[k])
        )
        copies[-1].start()
    for copy in copies:
        copy.wait()


def pick_kernel(flag, after, far, own, out):
    @pl.when(flag[0] == 0)
    def _():
        out[...] = far[...]

    @pl.when(flag[0] == 1)
    def _():
        out[...] = own[...]


def join_kernel(flag, after, distant, handed, out):
    weight = 1.0 - flag[0].astype(jnp.float32)
    out[...] = distant[...] + weight * handed[...]


def slab_moments(moments, i, reach):
    count = moments.shape[1]
    ahead = moments[i, 0, 0]
    behind = moments[i, count - 1, 1]
    for k in range(1, count):
        ahead = ahead * reach + moments[i, k, 0]
        behind = behind * reach + moments[i, count - 1 - k, 1]
    return ahead, behind


def forward_kernel(base, counts, after, own, other, right_ref, left_ref, decay, *refs):
    spectrum, moments, mine = refs
    owned, rows, side, width = own.shape
    chunks = rows // GROUP
    lower = lax.broadcasted_iota(jnp.int32, (side, width), 1) < width // 2

    def orbital_step(i, carry):
        live = count_at(counts, base + i) > 0

        def chunk_step(c, carry):
            block = pl.ds(pl.multiple_of(c * GROUP, GROUP), GROUP)
            density = own[i, block] * other[block]
            value = along_last(density.reshape(GROUP * side, width), right_ref[...])
            planes = [value[k * side : (k + 1) * side] for k in range(GROUP)]
            planes = along_second(planes, left_ref[...])
            ratio = decay[0]
            ahead = planes[0]
            behind = planes[-1]
            for k in range(GROUP):
                spectrum[i, c * GROUP + k] = planes[k]
                if k:
                    ahead = ahead * ratio + planes[k]
                    behind = behind * ratio + planes[GROUP - 1 - k]
            moments[i, c, 0] = ahead
            moments[i, c, 1] = behind
            return carry

        lax.fori_loop(0, jnp.where(live, chunks, 0), chunk_step, 0)

        @pl.when(live)
        def _():
            power = decay[1]
            ahead, behind = slab_moments(moments, i, decay[4])
            mine[i] = jnp.where(lower, behind + power * halves(behind), ahead + power * halves(ahead))

        return carry

    lax.fori_loop(0, owned, orbital_step, 0)


def backward_kernel(
    base, inside, counts, after, own, other, spectrum, moments, mine, arrived,
    right_ref, left_ref, decay, *refs
):
    edge = refs[-1]
    if inside:
        before, total = refs[:2]
        total[...] = before[...]
    else:
        total, partner = refs[-3:-1]
        total[...] = refs[0][...] if len(refs) > 3 else jnp.zeros_like(total)
        partner[...] = jnp.zeros_like(partner)
    owned, rows, side, width = own.shape
    chunks = rows // GROUP
    lower = lax.broadcasted_iota(jnp.int32, (side, width), 1) < width // 2

    def orbital_step(i, carry):
        number = count_at(counts, base + i)

        @pl.when(number > 0)
        def _():
            power, reach = decay[1], decay[4]
            ahead_all, behind_all = slab_moments(moments, i, reach)
            entering = (arrived[i] + power * power * mine[i]) * decay[3]
            turned = halves(entering)
            ahead = jnp.where(lower, turned, halves(ahead_all) + power * entering)
            behind = jnp.where(lower, halves(behind_all) + power * entering, turned)
            edge[0, 0] = ahead
            edge[chunks - 1, 1] = behind
            for k in range(1, chunks):
                ahead = ahead * reach + moments[i, k - 1, 0]
                edge[k, 0] = ahead
                behind = behind * reach + moments[i, chunks - k, 1]
                edge[chunks - 1 - k, 1] = behind

        def chunk_step(c, carry):
            block = pl.ds(pl.multiple_of(c * GROUP, GROUP), GROUP)
            ratio = decay[0]
            scale = decay[2] * number.astype(jnp.float32)
            ahead = edge[c, 0]
            behind = edge[c, 1]
            tails = []
            for k in reversed(range(GROUP)):
                spilled = ratio * behind
                tails.insert(0, spilled)
                behind = spectrum[i, c * GROUP + k] + spilled
            planes = []
            for k in range(GROUP):
                ahead = spectrum[i, c * GROUP + k] + ratio * ahead
                planes.append(scale * (ahead + tails[k]))
            planes = along_second(planes, left_ref[...])
            value = along_last(jnp.concatenate(planes, 0), right_ref[...])
            potential = value.reshape(GROUP, side, width)
            total[i, block] += potential * other[block]
            if inside:
                total[1, block] += potential * own[i, block]
            else:
                partner[block] += potential * own[i, block]
            return carry

        lax.fori_loop(0, jnp.where(number > 0, chunks, 0), chunk_step, 0)
        return carry

    lax.fori_loop(0, owned, orbital_step, 0)


def pair_counts(pair_list, pair_count, owned, band_index, band_count):
    first, partner = pair_list[0, :, 0], pair_list[0, :, 1]
    live = jnp.arange(first.shape[0]) < pair_count[0]
    distance = (partner // owned - band_index) % band_count
    inside = (REACH * owned) * owned
    place = ((partner % owned) * REACH + distance - 1) * owned + first
    place = jnp.where(distance == 0, inside, place)
    return jnp.sum(jnp.where(live, lax.shift_left(1, DIGIT * place), 0))


def count_at(counts, place):
    return lax.shift_right_logical(counts[0], 1 + DIGIT * place) & (2**DIGIT - 1)


def on_device(orbitals, pair_list, pair_count):
    owned, slab_rows, plane_cells = orbitals.shape
    side = math.isqrt(plane_cells)
    assert lax.axis_size("grid") == 2 and REACH == 2 and owned == 2
    rows = slab_rows // 2
    chunks = rows // GROUP
    band_count = lax.axis_size("band")
    band_index = lax.axis_index("band")
    right, left, decay = tables(side, rows)
    smem = pl.BlockSpec(memory_space=pltpu.SMEM)
    vmem = pl.BlockSpec(memory_space=pltpu.VMEM)
    free = pl.BlockSpec(memory_space=pl.ANY)
    hbm = pl.BlockSpec(memory_space=pltpu.HBM)
    params = pltpu.CompilerParams(vmem_limit_bytes=12 * 2**20)
    shape = (rows, side, 2 * side)
    one = jax.ShapeDtypeStruct(shape, jnp.float32)
    both = jax.ShapeDtypeStruct((owned,) + shape, jnp.float32)

    def call(kernel, out_shape, in_specs, out_specs=vmem, scratch=(), aliases={}):
        if isinstance(out_shape, tuple):
            out_specs = (vmem,) * len(out_shape)
        return pl.pallas_call(
            kernel,
            out_shape=out_shape,
            in_specs=in_specs,
            out_specs=out_specs,
            scratch_shapes=scratch,
            compiler_params=params,
            input_output_aliases=aliases,
            cost_estimate=pl.CostEstimate(flops=0, bytes_accessed=1 << 20, transcendentals=0),
        )

    source = pltpu.with_memory_space_constraint(orbitals, pltpu.HBM)
    fields, far = [], []
    for row in range(owned):
        field = call(
            functools.partial(arrange_kernel, row),
            one,
            [hbm] + [free] * row,
            scratch=[
                pltpu.VMEM(orbitals.shape[1:], jnp.float32),
                pltpu.SemaphoreType.DMA((PARTS,)),
            ],
        )(source, *fields)
        fields.append(field)
        far.append(rotated(field, "band", -2))
    own = call(stack_kernel, both, [vmem, vmem])(*fields)
    flag = (band_index % 2).reshape(1)
    counts = pair_counts(pair_list, pair_count, owned, band_index, band_count)
    counts = (lax.optimization_barrier(counts) * 2 + band_index % 2).reshape(1)

    def forward(base, after, other):
        return call(
            functools.partial(forward_kernel, base),
            (
                both,
                jax.ShapeDtypeStruct((owned, chunks, 2) + shape[1:], jnp.float32),
                jax.ShapeDtypeStruct((owned,) + shape[1:], jnp.float32),
            ),
            [smem, free] + [vmem] * 5,
        )(counts, after, own, other, right, left, decay)

    def exchanged(mine):
        return swapped(mine, "grid")

    def backward(base, after, state, total, inside=False):
        return call(
            functools.partial(backward_kernel, base, inside),
            both if inside else (both, one),
            [smem, free] + [vmem] * (9 + len(total)),
            scratch=[pltpu.VMEM((chunks, 2) + shape[1:], jnp.float32)],
        )(counts, after, own, *state, right, left, decay, *total)

    inner_base = REACH * owned * owned
    spectrum, moments, mine = forward(inner_base, own, fields[1])
    inner = (fields[1], spectrum, moments, mine, exchanged(mine))
    after = mine

    def brought(row, after):
        picked = call(pick_kernel, one, [smem, free, vmem, vmem])(
            flag, after, far[row], fields[row]
        )
        return picked, swapped(picked, "band")

    total, passed, arrived = (), [], []
    after, near = brought(0, after)
    for row in range(owned):
        base = row * REACH * owned
        distant_state = forward(base + owned, after, far[row])
        distant_ends = exchanged(distant_state[2])
        near_state = forward(base, distant_state[2], near)
        mine = near_state[2]
        near_state = (near,) + tuple(near_state) + (exchanged(mine),)
        distant_state = (far[row],) + tuple(distant_state) + (distant_ends,)
        acc, handed = backward(base, mine, near_state, total)
        handed_over = swapped(handed, "band")
        acc, distant = backward(base + owned, handed, distant_state, (acc,))
        total = (acc,)
        joined = call(join_kernel, one, [smem, free, vmem, vmem])(
            flag, distant, distant, handed_over
        )
        passed.append(handed_over)
        arrived.append(rotated(joined, "band", 2))
        after = joined
        if row + 1 < owned:
            after, near = brought(row + 1, joined)
    total = backward(inner_base, after, inner, total, inside=True)
    out = jax.ShapeDtypeStruct(orbitals.shape, jnp.float32)
    result = None
    for row in range(owned):
        earlier = [] if result is None else [result]
        result = call(
            functools.partial(restore_kernel, row),
            out,
            [smem] + [vmem] * 3 + [hbm] * len(earlier),
            out_specs=hbm,
            scratch=[
                pltpu.VMEM(orbitals.shape[1:], jnp.float32),
                pltpu.SemaphoreType.DMA((PARTS,)),
            ],
            aliases={4: 0} if earlier else {},
        )(flag, total, passed[row], arrived[row], *earlier)
    return result


def solution(mesh):
    in_specs = (P("band", "grid", None), P("band", None, None), P("band"))
    out_specs = P("band", "grid", None)

    return jax.shard_map(
        on_device, mesh=mesh, in_specs=in_specs, out_specs=out_specs, check_vma=False
    )
```

```python
import functools
import math

import jax
import jax.numpy as jnp
import numpy as np
from jax import lax
from jax.experimental import pallas as pl
from jax.experimental.pallas import tpu as pltpu
from jax.sharding import PartitionSpec as P

REACH = 2
GROUP = 8


def rotated(value, axis, steps):
    count = lax.axis_size(axis)
    pairs = [(source, (source + steps) % count) for source in range(count)]
    return lax.ppermute(value, axis, pairs)


def swapped(value, axis):
    count = lax.axis_size(axis)
    return lax.ppermute(value, axis, [(source, source ^ 1) for source in range(count)])


def split(value):
    high = value.astype(jnp.bfloat16)
    return high, (value - high.astype(jnp.float32)).astype(jnp.bfloat16)


def tables(side, half_rows):
    points = np.arange(side)
    angles = (points[:, None] * points[None, :] % side) * (2.0 * math.pi / side)
    hartley = (np.cos(angles) + np.sin(angles)).astype(np.float32)
    high = hartley.astype(jnp.bfloat16)
    low = (hartley - high.astype(np.float32)).astype(jnp.bfloat16)
    eye = np.eye(2, dtype=np.float32)
    wide_high = np.kron(eye, high.astype(np.float32))
    wide_low = np.kron(eye, low.astype(np.float32))
    right = np.block([[wide_high, wide_low], [wide_high, wide_low]]).astype(jnp.bfloat16)
    order = np.concatenate([points[0::2], points[1::2]])
    left = np.concatenate([part[order][:, order] for part in (high, high, low)], 1)
    eigenvalues = 2.0 - 2.0 * np.cos(points * (2.0 * math.pi / side))
    shift = 1.0 / side**2 + eigenvalues[order][:, None] + np.tile(eigenvalues, 2)[None, :]
    ratio = 1.0 + shift / 2 - np.sqrt(shift + shift**2 / 4)
    power = ratio**half_rows
    reach = ratio**GROUP
    scale = 1.0 / side / (1.0 / ratio - ratio) / side**2
    wrap = 1.0 / (1.0 - power**4)
    decay = np.stack([ratio, power, scale, wrap, reach]).astype(np.float32)
    return right, left, decay


def along_last(value, right):
    width = value.shape[1]
    product = jnp.dot(
        jnp.concatenate(split(value), 1), right, preferred_element_type=jnp.float32
    )
    return product[:, :width] + product[:, width:]


def along_second(planes, left):
    width = planes[0].shape[1]
    out = []
    for start in range(0, len(planes), 2):
        both = jnp.concatenate(planes[start : start + 2], 1)
        high, low = split(both)
        stacked = jnp.concatenate([high, low, high], 0)
        product = jnp.dot(left, stacked, preferred_element_type=jnp.float32)
        out.append(product[:, :width])
        out.append(product[:, width:])
    return out


def halves(value):
    return pltpu.roll(value, value.shape[-1] // 2, axis=value.ndim - 1)


DIGIT = 3


def tiled(value, width):
    count, slab_rows, cells = value.shape
    value = value.reshape(count, slab_rows // GROUP, GROUP, cells // width, width)
    return jnp.transpose(value, (0, 1, 3, 2, 4))


def arrange_kernel(row, source, *refs):
    packed, raw, arrivals = refs[-3:]
    groups, tiles, lines, width = raw.shape
    flat = raw.reshape(groups * tiles * lines, width)
    lower = lax.broadcasted_iota(jnp.int32, (tiles, width), 1) < width // 2
    half = groups // 2
    copies = [
        pltpu.make_async_copy(source.at[row, g], raw.at[g], arrivals.at[g]) for g in range(groups)
    ]
    for g in range(half):
        copies[g].start()
        copies[g + half].start()
    for g in range(half):
        copies[g].wait()
        copies[g + half].wait()
        for k in range(lines):
            near = flat[pl.ds(g * tiles * lines + k, tiles, stride=lines), :]
            far = flat[pl.ds((g + half) * tiles * lines + k, tiles, stride=lines), :]
            packed[g * lines + k, :tiles] = jnp.where(lower, near, halves(far))
            packed[g * lines + k, tiles:] = jnp.where(lower, halves(near), far)


def stack_kernel(first, second, own):
    own[0] = first[...]
    own[1] = second[...]


def restore_kernel(row, flag, own, passed, arrived, *refs):
    out, raw, departures = refs[-3:]
    groups, tiles, lines, width = raw.shape
    flat = raw.reshape(groups * tiles * lines, width)
    lower = lax.broadcasted_iota(jnp.int32, (tiles, width), 1) < width // 2
    half = groups // 2
    weight = flag[0].astype(jnp.float32)
    copies = [
        pltpu.make_async_copy(raw.at[g], out.at[row, g], departures.at[g]) for g in range(groups)
    ]
    for g in range(half):
        for k in range(lines):
            plane = g * lines + k
            block = own[row, plane] + weight * passed[plane] + arrived[plane]
            even, odd = block[:tiles], block[tiles:]
            near = pl.ds(g * tiles * lines + k, tiles, stride=lines)
            far = pl.ds((g + half) * tiles * lines + k, tiles, stride=lines)
            flat[near, :] = jnp.where(lower, even, halves(odd))
            flat[far, :] = jnp.where(lower, halves(even), odd)
        copies[g].start()
        copies[g + half].start()
    for copy in copies:
        copy.wait()


def pick_kernel(flag, after, far, own, out):
    @pl.when(flag[0] == 0)
    def _():
        out[...] = far[...]

    @pl.when(flag[0] == 1)
    def _():
        out[...] = own[...]


def join_kernel(flag, after, distant, handed, out):
    weight = 1.0 - flag[0].astype(jnp.float32)
    out[...] = distant[...] + weight * handed[...]


def slab_moments(moments, i, reach):
    count = moments.shape[1]
    ahead = moments[i, 0, 0]
    behind = moments[i, count - 1, 1]
    for k in range(1, count):
        ahead = ahead * reach + moments[i, k, 0]
        behind = behind * reach + moments[i, count - 1 - k, 1]
    return ahead, behind


def forward_kernel(base, counts, after, own, other, right_ref, left_ref, decay, *refs):
    spectrum, moments, mine = refs
    owned, rows, side, width = own.shape
    chunks = rows // GROUP
    lower = lax.broadcasted_iota(jnp.int32, (side, width), 1) < width // 2

    def orbital_step(i, carry):
        live = count_at(counts, base + i) > 0

        def chunk_step(c, carry):
            block = pl.ds(pl.multiple_of(c * GROUP, GROUP), GROUP)
            density = own[i, block] * other[block]
            value = along_last(density.reshape(GROUP * side, width), right_ref[...])
            planes = [value[k * side : (k + 1) * side] for k in range(GROUP)]
            planes = along_second(planes, left_ref[...])
            ratio = decay[0]
            ahead = planes[0]
            behind = planes[-1]
            for k in range(GROUP):
                spectrum[i, c * GROUP + k] = planes[k]
                if k:
                    ahead = ahead * ratio + planes[k]
                    behind = behind * ratio + planes[GROUP - 1 - k]
            moments[i, c, 0] = ahead
            moments[i, c, 1] = behind
            return carry

        lax.fori_loop(0, jnp.where(live, chunks, 0), chunk_step, 0)

        @pl.when(live)
        def _():
            power = decay[1]
            ahead, behind = slab_moments(moments, i, decay[4])
            mine[i] = jnp.where(lower, behind + power * halves(behind), ahead + power * halves(ahead))

        return carry

    lax.fori_loop(0, owned, orbital_step, 0)


def backward_kernel(
    base, inside, counts, after, own, other, spectrum, moments, mine, arrived,
    right_ref, left_ref, decay, *refs
):
    edge = refs[-1]
    if inside:
        before, total = refs[:2]
        total[...] = before[...]
    else:
        total, partner = refs[-3:-1]
        total[...] = refs[0][...] if len(refs) > 3 else jnp.zeros_like(total)
        partner[...] = jnp.zeros_like(partner)
    owned, rows, side, width = own.shape
    chunks = rows // GROUP
    lower = lax.broadcasted_iota(jnp.int32, (side, width), 1) < width // 2

    def orbital_step(i, carry):
        number = count_at(counts, base + i)

        @pl.when(number > 0)
        def _():
            power, reach = decay[1], decay[4]
            ahead_all, behind_all = slab_moments(moments, i, reach)
            entering = (arrived[i] + power * power * mine[i]) * decay[3]
            turned = halves(entering)
            ahead = jnp.where(lower, turned, halves(ahead_all) + power * entering)
            behind = jnp.where(lower, halves(behind_all) + power * entering, turned)
            edge[0, 0] = ahead
            edge[chunks - 1, 1] = behind
            for k in range(1, chunks):
                ahead = ahead * reach + moments[i, k - 1, 0]
                edge[k, 0] = ahead
                behind = behind * reach + moments[i, chunks - k, 1]
                edge[chunks - 1 - k, 1] = behind

        def chunk_step(c, carry):
            block = pl.ds(pl.multiple_of(c * GROUP, GROUP), GROUP)
            ratio = decay[0]
            scale = decay[2] * number.astype(jnp.float32)
            ahead = edge[c, 0]
            behind = edge[c, 1]
            tails = []
            for k in reversed(range(GROUP)):
                spilled = ratio * behind
                tails.insert(0, spilled)
                behind = spectrum[i, c * GROUP + k] + spilled
            planes = []
            for k in range(GROUP):
                ahead = spectrum[i, c * GROUP + k] + ratio * ahead
                planes.append(scale * (ahead + tails[k]))
            planes = along_second(planes, left_ref[...])
            value = along_last(jnp.concatenate(planes, 0), right_ref[...])
            potential = value.reshape(GROUP, side, width)
            total[i, block] += potential * other[block]
            if inside:
                total[1, block] += potential * own[i, block]
            else:
                partner[block] += potential * own[i, block]
            return carry

        lax.fori_loop(0, jnp.where(number > 0, chunks, 0), chunk_step, 0)
        return carry

    lax.fori_loop(0, owned, orbital_step, 0)


def pair_counts(pair_list, pair_count, owned, band_index, band_count):
    first, partner = pair_list[0, :, 0], pair_list[0, :, 1]
    live = jnp.arange(first.shape[0]) < pair_count[0]
    distance = (partner // owned - band_index) % band_count
    inside = (REACH * owned) * owned
    place = ((partner % owned) * REACH + distance - 1) * owned + first
    place = jnp.where(distance == 0, inside, place)
    return jnp.sum(jnp.where(live, lax.shift_left(1, DIGIT * place), 0))


def count_at(counts, place):
    return lax.shift_right_logical(counts[0], 1 + DIGIT * place) & (2**DIGIT - 1)


def on_device(orbitals, pair_list, pair_count):
    owned, slab_rows, plane_cells = orbitals.shape
    side = math.isqrt(plane_cells)
    assert lax.axis_size("grid") == 2 and REACH == 2 and owned == 2
    rows = slab_rows // 2
    chunks = rows // GROUP
    band_count = lax.axis_size("band")
    band_index = lax.axis_index("band")
    right, left, decay = tables(side, rows)
    smem = pl.BlockSpec(memory_space=pltpu.SMEM)
    vmem = pl.BlockSpec(memory_space=pltpu.VMEM)
    free = pl.BlockSpec(memory_space=pl.ANY)
    hbm = pl.BlockSpec(memory_space=pltpu.HBM)
    params = pltpu.CompilerParams(vmem_limit_bytes=12 * 2**20)
    shape = (rows, side, 2 * side)
    one = jax.ShapeDtypeStruct(shape, jnp.float32)
    both = jax.ShapeDtypeStruct((owned,) + shape, jnp.float32)

    def call(kernel, out_shape, in_specs, out_specs=vmem, scratch=(), aliases={}):
        if isinstance(out_shape, tuple):
            out_specs = (vmem,) * len(out_shape)
        return pl.pallas_call(
            kernel,
            out_shape=out_shape,
            in_specs=in_specs,
            out_specs=out_specs,
            scratch_shapes=scratch,
            compiler_params=params,
            input_output_aliases=aliases,
            cost_estimate=pl.CostEstimate(flops=0, bytes_accessed=1 << 20, transcendentals=0),
        )

    tiles = tiled(orbitals, 2 * side)
    source = pltpu.with_memory_space_constraint(tiles, pltpu.HBM)
    fields, far = [], []
    for row in range(owned):
        field = call(
            functools.partial(arrange_kernel, row),
            one,
            [hbm] + [free] * row,
            scratch=[
                pltpu.VMEM(tiles.shape[1:], jnp.float32),
                pltpu.SemaphoreType.DMA(tiles.shape[1:2]),
            ],
        )(source, *fields)
        fields.append(field)
        far.append(rotated(field, "band", -2))
    own = call(stack_kernel, both, [vmem, vmem])(*fields)
    flag = (band_index % 2).reshape(1)
    counts = pair_counts(pair_list, pair_count, owned, band_index, band_count)
    counts = (lax.optimization_barrier(counts) * 2 + band_index % 2).reshape(1)

    def forward(base, after, other):
        return call(
            functools.partial(forward_kernel, base),
            (
                both,
                jax.ShapeDtypeStruct((owned, chunks, 2) + shape[1:], jnp.float32),
                jax.ShapeDtypeStruct((owned,) + shape[1:], jnp.float32),
            ),
            [smem, free] + [vmem] * 5,
        )(counts, after, own, other, right, left, decay)

    def exchanged(mine):
        return swapped(mine, "grid")

    def backward(base, after, state, total, inside=False):
        return call(
            functools.partial(backward_kernel, base, inside),
            both if inside else (both, one),
            [smem, free] + [vmem] * (9 + len(total)),
            scratch=[pltpu.VMEM((chunks, 2) + shape[1:], jnp.float32)],
        )(counts, after, own, *state, right, left, decay, *total)

    inner_base = REACH * owned * owned
    spectrum, moments, mine = forward(inner_base, own, fields[1])
    inner = (fields[1], spectrum, moments, mine, exchanged(mine))
    after = mine

    def brought(row, after):
        picked = call(pick_kernel, one, [smem, free, vmem, vmem])(
            flag, after, far[row], fields[row]
        )
        return picked, swapped(picked, "band")

    total, passed, arrived = (), [], []
    after, near = brought(0, after)
    for row in range(owned):
        base = row * REACH * owned
        distant_state = forward(base + owned, after, far[row])
        distant_ends = exchanged(distant_state[2])
        near_state = forward(base, distant_state[2], near)
        mine = near_state[2]
        near_state = (near,) + tuple(near_state) + (exchanged(mine),)
        distant_state = (far[row],) + tuple(distant_state) + (distant_ends,)
        acc, handed = backward(base, mine, near_state, total)
        handed_over = swapped(handed, "band")
        acc, distant = backward(base + owned, handed, distant_state, (acc,))
        total = (acc,)
        joined = call(join_kernel, one, [smem, free, vmem, vmem])(
            flag, distant, distant, handed_over
        )
        passed.append(handed_over)
        arrived.append(rotated(joined, "band", 2))
        after = joined
        if row + 1 < owned:
            after, near = brought(row + 1, joined)
    total = backward(inner_base, after, inner, total, inside=True)
    out = jax.ShapeDtypeStruct(tiles.shape, jnp.float32)
    result = None
    for row in range(owned):
        earlier = [] if result is None else [result]
        result = call(
            functools.partial(restore_kernel, row),
            out,
            [smem] + [vmem] * 3 + [hbm] * len(earlier),
            out_specs=hbm,
            scratch=[
                pltpu.VMEM(tiles.shape[1:], jnp.float32),
                pltpu.SemaphoreType.DMA(tiles.shape[1:2]),
            ],
            aliases={4: 0} if earlier else {},
        )(flag, total, passed[row], arrived[row], *earlier)
    return jnp.transpose(result, (0, 1, 3, 2, 4)).reshape(orbitals.shape)


def solution(mesh):
    in_specs = (P("band", "grid", None), P("band", None, None), P("band"))
    out_specs = P("band", "grid", None)

    return jax.shard_map(
        on_device, mesh=mesh, in_specs=in_specs, out_specs=out_specs, check_vma=False
    )
```

```python
import functools
import math

import jax
import jax.numpy as jnp
import numpy as np
from jax import lax
from jax.experimental import pallas as pl
from jax.experimental.pallas import tpu as pltpu
from jax.sharding import PartitionSpec as P

REACH = 2
GROUP = 8


def rotated(value, axis, steps, parity):
    count = lax.axis_size(axis)
    sources = range(parity, count, 2)
    return lax.ppermute(value, axis, [(source, (source + steps) % count) for source in sources])


def swapped(value, axis, parities=(0, 1)):
    count = lax.axis_size(axis)
    sources = [source for source in range(count) if source % 2 in parities]
    return lax.ppermute(value, axis, [(source, source ^ 1) for source in sources])


def split(value):
    high = value.astype(jnp.bfloat16)
    return high, (value - high.astype(jnp.float32)).astype(jnp.bfloat16)


def tables(side, half_rows):
    points = np.arange(side)
    angles = (points[:, None] * points[None, :] % side) * (2.0 * math.pi / side)
    hartley = (np.cos(angles) + np.sin(angles)).astype(np.float32)
    high = hartley.astype(jnp.bfloat16)
    low = (hartley - high.astype(np.float32)).astype(jnp.bfloat16)
    eye = np.eye(2, dtype=np.float32)
    wide_high = np.kron(eye, high.astype(np.float32))
    wide_low = np.kron(eye, low.astype(np.float32))
    right = np.block([[wide_high, wide_low], [wide_high, wide_low]]).astype(jnp.bfloat16)
    order = np.concatenate([points[0::2], points[1::2]])
    left = np.concatenate([part[order][:, order] for part in (high, high, low)], 1)
    eigenvalues = 2.0 - 2.0 * np.cos(points * (2.0 * math.pi / side))
    shift = 1.0 / side**2 + eigenvalues[order][:, None] + np.tile(eigenvalues, 2)[None, :]
    ratio = 1.0 + shift / 2 - np.sqrt(shift + shift**2 / 4)
    power = ratio**half_rows
    reach = ratio**GROUP
    scale = 1.0 / side / (1.0 / ratio - ratio) / side**2
    wrap = 1.0 / (1.0 - power**4)
    decay = np.stack([ratio, power, scale, wrap, reach]).astype(np.float32)
    return right, left, decay


def along_last(value, right):
    width = value.shape[1]
    product = jnp.dot(
        jnp.concatenate(split(value), 1), right, preferred_element_type=jnp.float32
    )
    return product[:, :width] + product[:, width:]


def along_second(planes, left):
    width = planes[0].shape[1]
    out = []
    for start in range(0, len(planes), 2):
        both = jnp.concatenate(planes[start : start + 2], 1)
        high, low = split(both)
        stacked = jnp.concatenate([high, low, high], 0)
        product = jnp.dot(left, stacked, preferred_element_type=jnp.float32)
        out.append(product[:, :width])
        out.append(product[:, width:])
    return out


def halves(value):
    return pltpu.roll(value, value.shape[-1] // 2, axis=value.ndim - 1)


DIGIT = 3


def tiled(value, width):
    count, slab_rows, cells = value.shape
    value = value.reshape(count, slab_rows // GROUP, GROUP, cells // width, width)
    return jnp.transpose(value, (0, 1, 3, 2, 4))


def arrange_kernel(row, source, *refs):
    packed, raw, arrivals = refs[-3:]
    groups, tiles, lines, width = raw.shape
    flat = raw.reshape(groups * tiles * lines, width)
    lower = lax.broadcasted_iota(jnp.int32, (tiles, width), 1) < width // 2
    half = groups // 2
    copies = [
        pltpu.make_async_copy(source.at[row, g], raw.at[g], arrivals.at[g]) for g in range(groups)
    ]
    for g in range(half):
        copies[g].start()
        copies[g + half].start()
    for g in range(half):
        copies[g].wait()
        copies[g + half].wait()
        for k in range(lines):
            near = flat[pl.ds(g * tiles * lines + k, tiles, stride=lines), :]
            far = flat[pl.ds((g + half) * tiles * lines + k, tiles, stride=lines), :]
            packed[g * lines + k, :tiles] = jnp.where(lower, near, halves(far))
            packed[g * lines + k, tiles:] = jnp.where(lower, halves(near), far)


def stack_kernel(first, second, own):
    own[0] = first[...]
    own[1] = second[...]


def restore_kernel(row, own, *refs):
    terms = refs[:3]
    out, raw, departures = refs[-3:]
    groups, tiles, lines, width = raw.shape
    flat = raw.reshape(groups * tiles * lines, width)
    lower = lax.broadcasted_iota(jnp.int32, (tiles, width), 1) < width // 2
    half = groups // 2
    copies = [
        pltpu.make_async_copy(raw.at[g], out.at[row, g], departures.at[g]) for g in range(groups)
    ]
    for g in range(half):
        for k in range(lines):
            plane = g * lines + k
            block = own[row, plane]
            for term in terms:
                block = block + term[plane]
            even, odd = block[:tiles], block[tiles:]
            near = pl.ds(g * tiles * lines + k, tiles, stride=lines)
            far = pl.ds((g + half) * tiles * lines + k, tiles, stride=lines)
            flat[near, :] = jnp.where(lower, even, halves(odd))
            flat[far, :] = jnp.where(lower, halves(even), odd)
        copies[g].start()
        copies[g + half].start()
    for copy in copies:
        copy.wait()


def pick_kernel(counts, after, even, odd, out):
    @pl.when(counts[0] & 1 == 0)
    def _():
        out[...] = even[...]

    @pl.when(counts[0] & 1 == 1)
    def _():
        out[...] = odd[...]


def join_kernel(after, distant, handed, out):
    out[...] = distant[...] + handed[...]


def slab_moments(moments, i, reach):
    count = moments.shape[1]
    ahead = moments[i, 0, 0]
    behind = moments[i, count - 1, 1]
    for k in range(1, count):
        ahead = ahead * reach + moments[i, k, 0]
        behind = behind * reach + moments[i, count - 1 - k, 1]
    return ahead, behind


def forward_kernel(base, counts, after, own, other, right_ref, left_ref, decay, *refs):
    spectrum, moments, mine = refs
    owned, rows, side, width = own.shape
    chunks = rows // GROUP
    lower = lax.broadcasted_iota(jnp.int32, (side, width), 1) < width // 2

    def orbital_step(i, carry):
        live = count_at(counts, base + i) > 0

        def chunk_step(c, carry):
            block = pl.ds(pl.multiple_of(c * GROUP, GROUP), GROUP)
            density = own[i, block] * other[block]
            value = along_last(density.reshape(GROUP * side, width), right_ref[...])
            planes = [value[k * side : (k + 1) * side] for k in range(GROUP)]
            planes = along_second(planes, left_ref[...])
            ratio = decay[0]
            ahead = planes[0]
            behind = planes[-1]
            for k in range(GROUP):
                spectrum[i, c * GROUP + k] = planes[k]
                if k:
                    ahead = ahead * ratio + planes[k]
                    behind = behind * ratio + planes[GROUP - 1 - k]
            moments[i, c, 0] = ahead
            moments[i, c, 1] = behind
            return carry

        lax.fori_loop(0, jnp.where(live, chunks, 0), chunk_step, 0)

        @pl.when(live)
        def _():
            power = decay[1]
            ahead, behind = slab_moments(moments, i, decay[4])
            mine[i] = jnp.where(lower, behind + power * halves(behind), ahead + power * halves(ahead))

        return carry

    lax.fori_loop(0, owned, orbital_step, 0)


def backward_kernel(
    base, inside, counts, after, own, other, spectrum, moments, mine, arrived,
    right_ref, left_ref, decay, *refs
):
    edge = refs[-1]
    if inside:
        before, total = refs[:2]
        total[...] = before[...]
    else:
        total, partner = refs[-3:-1]
        total[...] = refs[0][...] if len(refs) > 3 else jnp.zeros_like(total)
        partner[...] = jnp.zeros_like(partner)
    owned, rows, side, width = own.shape
    chunks = rows // GROUP
    lower = lax.broadcasted_iota(jnp.int32, (side, width), 1) < width // 2

    def orbital_step(i, carry):
        number = count_at(counts, base + i)

        @pl.when(number > 0)
        def _():
            power, reach = decay[1], decay[4]
            ahead_all, behind_all = slab_moments(moments, i, reach)
            entering = (arrived[i] + power * power * mine[i]) * decay[3]
            turned = halves(entering)
            ahead = jnp.where(lower, turned, halves(ahead_all) + power * entering)
            behind = jnp.where(lower, halves(behind_all) + power * entering, turned)
            edge[0, 0] = ahead
            edge[chunks - 1, 1] = behind
            for k in range(1, chunks):
                ahead = ahead * reach + moments[i, k - 1, 0]
                edge[k, 0] = ahead
                behind = behind * reach + moments[i, chunks - k, 1]
                edge[chunks - 1 - k, 1] = behind

        def chunk_step(c, carry):
            block = pl.ds(pl.multiple_of(c * GROUP, GROUP), GROUP)
            ratio = decay[0]
            scale = decay[2] * number.astype(jnp.float32)
            ahead = edge[c, 0]
            behind = edge[c, 1]
            tails = []
            for k in reversed(range(GROUP)):
                spilled = ratio * behind
                tails.insert(0, spilled)
                behind = spectrum[i, c * GROUP + k] + spilled
            planes = []
            for k in range(GROUP):
                ahead = spectrum[i, c * GROUP + k] + ratio * ahead
                planes.append(scale * (ahead + tails[k]))
            planes = along_second(planes, left_ref[...])
            value = along_last(jnp.concatenate(planes, 0), right_ref[...])
            potential = value.reshape(GROUP, side, width)
            total[i, block] += potential * other[block]
            if inside:
                total[1, block] += potential * own[i, block]
            else:
                partner[block] += potential * own[i, block]
            return carry

        lax.fori_loop(0, jnp.where(number > 0, chunks, 0), chunk_step, 0)
        return carry

    lax.fori_loop(0, owned, orbital_step, 0)


def pair_counts(pair_list, pair_count, owned, band_index, band_count):
    first, partner = pair_list[0, :, 0], pair_list[0, :, 1]
    live = jnp.arange(first.shape[0]) < pair_count[0]
    distance = (partner // owned - band_index) % band_count
    inside = (REACH * owned) * owned
    side = jnp.where(distance == REACH - band_index % 2, 0, 1)
    place = ((partner % owned) * REACH + side) * owned + first
    place = jnp.where(distance == 0, inside, place)
    return jnp.sum(jnp.where(live, lax.shift_left(1, DIGIT * place), 0))


def count_at(counts, place):
    return lax.shift_right_logical(counts[0], 1 + DIGIT * place) & (2**DIGIT - 1)


def on_device(orbitals, pair_list, pair_count):
    owned, slab_rows, plane_cells = orbitals.shape
    side = math.isqrt(plane_cells)
    assert lax.axis_size("grid") == 2 and REACH == 2 and owned == 2
    rows = slab_rows // 2
    chunks = rows // GROUP
    band_count = lax.axis_size("band")
    band_index = lax.axis_index("band")
    right, left, decay = tables(side, rows)
    smem = pl.BlockSpec(memory_space=pltpu.SMEM)
    vmem = pl.BlockSpec(memory_space=pltpu.VMEM)
    free = pl.BlockSpec(memory_space=pl.ANY)
    hbm = pl.BlockSpec(memory_space=pltpu.HBM)
    params = pltpu.CompilerParams(vmem_limit_bytes=12 * 2**20)
    shape = (rows, side, 2 * side)
    one = jax.ShapeDtypeStruct(shape, jnp.float32)
    both = jax.ShapeDtypeStruct((owned,) + shape, jnp.float32)

    def call(kernel, out_shape, in_specs, out_specs=vmem, scratch=(), aliases={}):
        if isinstance(out_shape, tuple):
            out_specs = (vmem,) * len(out_shape)
        return pl.pallas_call(
            kernel,
            out_shape=out_shape,
            in_specs=in_specs,
            out_specs=out_specs,
            scratch_shapes=scratch,
            compiler_params=params,
            input_output_aliases=aliases,
            cost_estimate=pl.CostEstimate(flops=0, bytes_accessed=1 << 20, transcendentals=0),
        )

    tiles = tiled(orbitals, 2 * side)
    source = pltpu.with_memory_space_constraint(tiles, pltpu.HBM)
    fields, leading, neighbour = [], [], []
    for row in range(owned):
        field = call(
            functools.partial(arrange_kernel, row),
            one,
            [hbm] + [free] * row,
            scratch=[
                pltpu.VMEM(tiles.shape[1:], jnp.float32),
                pltpu.SemaphoreType.DMA(tiles.shape[1:2]),
            ],
        )(source, *fields)
        fields.append(field)
        leading.append(rotated(field, "band", -2, 0))
        neighbour.append(swapped(field, "band", (1,)))
    own = call(stack_kernel, both, [vmem, vmem])(*fields)
    counts = pair_counts(pair_list, pair_count, owned, band_index, band_count)
    counts = (lax.optimization_barrier(counts) * 2 + band_index % 2).reshape(1)

    def forward(base, after, other):
        return call(
            functools.partial(forward_kernel, base),
            (
                both,
                jax.ShapeDtypeStruct((owned, chunks, 2) + shape[1:], jnp.float32),
                jax.ShapeDtypeStruct((owned,) + shape[1:], jnp.float32),
            ),
            [smem, free] + [vmem] * 5,
        )(counts, after, own, other, right, left, decay)

    def exchanged(mine):
        return swapped(mine, "grid")

    def backward(base, after, state, total, inside=False):
        return call(
            functools.partial(backward_kernel, base, inside),
            both if inside else (both, one),
            [smem, free] + [vmem] * (9 + len(total)),
            scratch=[pltpu.VMEM((chunks, 2) + shape[1:], jnp.float32)],
        )(counts, after, own, *state, right, left, decay, *total)

    def chosen(after, even, odd):
        return call(pick_kernel, one, [smem, free, vmem, vmem])(counts, after, even, odd)

    def solved(base, after, other):
        spectrum, moments, mine = forward(base, after, other)
        return (other, spectrum, moments, mine, exchanged(mine))

    def joined(after, mine, handed):
        return call(join_kernel, one, [free, vmem, vmem])(after, mine, handed)

    def sent(value, steps, parity):
        return rotated(value, "band", steps, parity)

    def crossed(value, parity):
        return swapped(value, "band", (parity,))

    inner_base = REACH * owned * owned
    step = REACH * owned
    inner = solved(inner_base, own, fields[1])
    copies = [crossed(leading[row], 0) for row in range(owned)]
    trailing = [sent(fields[row], -2, 1) for row in range(owned)]

    picked = chosen(inner[3], leading[0], copies[0])
    first = solved(0, picked, picked)
    total, first_part = backward(0, first[3], first, ())
    first_handed = crossed(first_part, 1)
    picked = chosen(first_part, leading[1], copies[1])
    second = solved(step, picked, picked)
    first_sum = joined(second[3], first_part, first_handed)
    lead_back = [sent(first_sum, 2, 0)]

    picked = chosen(first_sum, neighbour[0], trailing[0])
    third = solved(owned, picked, picked)
    total, second_part = backward(step, third[3], second, (total,))
    second_handed = crossed(second_part, 1)
    second_sum = joined(second_part, second_part, second_handed)
    lead_back.append(sent(second_sum, 2, 0))

    picked = chosen(second_sum, neighbour[1], trailing[1])
    fourth = solved(step + owned, picked, picked)
    total, third_part = backward(owned, fourth[3], third, (total,))
    trail_back = [sent(third_part, 2, 1)]
    given = [crossed(third_part, 0)]
    total, fourth_part = backward(step + owned, third_part, fourth, (total,))
    trail_back.append(sent(fourth_part, 2, 1))
    given.append(crossed(fourth_part, 0))
    total = backward(inner_base, fourth_part, inner, (total,), inside=True)
    out = jax.ShapeDtypeStruct(tiles.shape, jnp.float32)
    result = None
    for row in range(owned):
        earlier = [] if result is None else [result]
        result = call(
            functools.partial(restore_kernel, row),
            out,
            [vmem] * 4 + [hbm] * len(earlier),
            out_specs=hbm,
            scratch=[
                pltpu.VMEM(tiles.shape[1:], jnp.float32),
                pltpu.SemaphoreType.DMA(tiles.shape[1:2]),
            ],
            aliases={4: 0} if earlier else {},
        )(total, given[row], lead_back[row], trail_back[row], *earlier)
    return jnp.transpose(result, (0, 1, 3, 2, 4)).reshape(orbitals.shape)


def solution(mesh):
    in_specs = (P("band", "grid", None), P("band", None, None), P("band"))
    out_specs = P("band", "grid", None)

    return jax.shard_map(
        on_device, mesh=mesh, in_specs=in_specs, out_specs=out_specs, check_vma=False
    )
```

```python
import functools
import math

import jax
import jax.numpy as jnp
import numpy as np
from jax import lax
from jax.experimental import pallas as pl
from jax.experimental.pallas import tpu as pltpu
from jax.sharding import PartitionSpec as P

REACH = 2
GROUP = 8


def rotated(value, axis, steps):
    count = lax.axis_size(axis)
    pairs = [(source, (source + steps) % count) for source in range(count)]
    return lax.ppermute(value, axis, pairs)


def swapped(value, axis):
    count = lax.axis_size(axis)
    return lax.ppermute(value, axis, [(source, source ^ 1) for source in range(count)])


def split(value):
    high = value.astype(jnp.bfloat16)
    return high, (value - high.astype(jnp.float32)).astype(jnp.bfloat16)


def tables(side, half_rows):
    points = np.arange(side)
    angles = (points[:, None] * points[None, :] % side) * (2.0 * math.pi / side)
    hartley = (np.cos(angles) + np.sin(angles)).astype(np.float32)
    high = hartley.astype(jnp.bfloat16)
    low = (hartley - high.astype(np.float32)).astype(jnp.bfloat16)
    eye = np.eye(2, dtype=np.float32)
    wide_high = np.kron(eye, high.astype(np.float32))
    wide_low = np.kron(eye, low.astype(np.float32))
    right = np.block([[wide_high, wide_low], [wide_high, wide_low]]).astype(jnp.bfloat16)
    order = np.concatenate([points[0::2], points[1::2]])
    left = np.concatenate([part[order][:, order] for part in (high, high, low)], 1)
    eigenvalues = 2.0 - 2.0 * np.cos(points * (2.0 * math.pi / side))
    shift = 1.0 / side**2 + eigenvalues[order][:, None] + np.tile(eigenvalues, 2)[None, :]
    ratio = 1.0 + shift / 2 - np.sqrt(shift + shift**2 / 4)
    power = ratio**half_rows
    reach = ratio**GROUP
    scale = 1.0 / side / (1.0 / ratio - ratio) / side**2
    wrap = 1.0 / (1.0 - power**4)
    decay = np.stack([ratio, power, scale, wrap, reach]).astype(np.float32)
    return right, left, decay


def along_last(value, right):
    width = value.shape[1]
    product = jnp.dot(
        jnp.concatenate(split(value), 1), right, preferred_element_type=jnp.float32
    )
    return product[:, :width] + product[:, width:]


def along_second(planes, left):
    width = planes[0].shape[1]
    out = []
    for start in range(0, len(planes), 2):
        both = jnp.concatenate(planes[start : start + 2], 1)
        high, low = split(both)
        stacked = jnp.concatenate([high, low, high], 0)
        product = jnp.dot(left, stacked, preferred_element_type=jnp.float32)
        out.append(product[:, :width])
        out.append(product[:, width:])
    return out


def halves(value):
    return pltpu.roll(value, value.shape[-1] // 2, axis=value.ndim - 1)


DIGIT = 3


def tiled(value, width):
    count, slab_rows, cells = value.shape
    value = value.reshape(count, slab_rows // GROUP, GROUP, cells // width, width)
    return jnp.transpose(value, (0, 1, 3, 2, 4))


def arrange_kernel(row, source, *refs):
    packed, raw, arrivals = refs[-3:]
    groups, tiles, lines, width = raw.shape
    flat = raw.reshape(groups * tiles * lines, width)
    lower = lax.broadcasted_iota(jnp.int32, (tiles, width), 1) < width // 2
    half = groups // 2
    copies = [
        pltpu.make_async_copy(source.at[row, g], raw.at[g], arrivals.at[g]) for g in range(groups)
    ]
    for g in range(half):
        copies[g].start()
        copies[g + half].start()
    for g in range(half):
        copies[g].wait()
        copies[g + half].wait()
        for k in range(lines):
            near = flat[pl.ds(g * tiles * lines + k, tiles, stride=lines), :]
            far = flat[pl.ds((g + half) * tiles * lines + k, tiles, stride=lines), :]
            packed[g * lines + k, :tiles] = jnp.where(lower, near, halves(far))
            packed[g * lines + k, tiles:] = jnp.where(lower, halves(near), far)


def stack_kernel(first, second, own):
    own[0] = first[...]
    own[1] = second[...]


def restore_kernel(row, flag, own, passed, arrived, *refs):
    out, raw, departures = refs[-3:]
    groups, tiles, lines, width = raw.shape
    flat = raw.reshape(groups * tiles * lines, width)
    lower = lax.broadcasted_iota(jnp.int32, (tiles, width), 1) < width // 2
    half = groups // 2
    weight = 1.0 - flag[0].astype(jnp.float32)
    copies = [
        pltpu.make_async_copy(raw.at[g], out.at[row, g], departures.at[g]) for g in range(groups)
    ]
    for g in range(half):
        for k in range(lines):
            plane = g * lines + k
            block = own[row, plane] + weight * passed[plane] + arrived[plane]
            even, odd = block[:tiles], block[tiles:]
            near = pl.ds(g * tiles * lines + k, tiles, stride=lines)
            far = pl.ds((g + half) * tiles * lines + k, tiles, stride=lines)
            flat[near, :] = jnp.where(lower, even, halves(odd))
            flat[far, :] = jnp.where(lower, halves(even), odd)
        copies[g].start()
        copies[g + half].start()
    for copy in copies:
        copy.wait()


def pick_kernel(flag, after, own, far, out):
    @pl.when(flag[0] == 0)
    def _():
        out[...] = own[...]

    @pl.when(flag[0] == 1)
    def _():
        out[...] = far[...]


def join_kernel(flag, after, distant, handed, out):
    weight = flag[0].astype(jnp.float32)
    out[...] = distant[...] + weight * handed[...]


def slab_moments(moments, i, reach):
    count = moments.shape[1]
    ahead = moments[i, 0, 0]
    behind = moments[i, count - 1, 1]
    for k in range(1, count):
        ahead = ahead * reach + moments[i, k, 0]
        behind = behind * reach + moments[i, count - 1 - k, 1]
    return ahead, behind


def forward_kernel(base, counts, after, own, other, right_ref, left_ref, decay, *refs):
    spectrum, moments, mine = refs
    owned, rows, side, width = own.shape
    chunks = rows // GROUP
    lower = lax.broadcasted_iota(jnp.int32, (side, width), 1) < width // 2

    def orbital_step(i, carry):
        live = count_at(counts, base + i) > 0

        def chunk_step(c, carry):
            block = pl.ds(pl.multiple_of(c * GROUP, GROUP), GROUP)
            density = own[i, block] * other[block]
            value = along_last(density.reshape(GROUP * side, width), right_ref[...])
            planes = [value[k * side : (k + 1) * side] for k in range(GROUP)]
            planes = along_second(planes, left_ref[...])
            ratio = decay[0]
            ahead = planes[0]
            behind = planes[-1]
            for k in range(GROUP):
                spectrum[i, c * GROUP + k] = planes[k]
                if k:
                    ahead = ahead * ratio + planes[k]
                    behind = behind * ratio + planes[GROUP - 1 - k]
            moments[i, c, 0] = ahead
            moments[i, c, 1] = behind
            return carry

        lax.fori_loop(0, jnp.where(live, chunks, 0), chunk_step, 0)

        @pl.when(live)
        def _():
            power = decay[1]
            ahead, behind = slab_moments(moments, i, decay[4])
            mine[i] = jnp.where(lower, behind + power * halves(behind), ahead + power * halves(ahead))

        return carry

    lax.fori_loop(0, owned, orbital_step, 0)


def backward_kernel(
    base, inside, counts, after, own, other, spectrum, moments, mine, arrived,
    right_ref, left_ref, decay, *refs
):
    edge = refs[-1]
    if inside:
        before, total = refs[:2]
        total[...] = before[...]
    else:
        total, partner = refs[-3:-1]
        total[...] = refs[0][...] if len(refs) > 3 else jnp.zeros_like(total)
        partner[...] = jnp.zeros_like(partner)
    owned, rows, side, width = own.shape
    chunks = rows // GROUP
    lower = lax.broadcasted_iota(jnp.int32, (side, width), 1) < width // 2

    def orbital_step(i, carry):
        number = count_at(counts, base + i)

        @pl.when(number > 0)
        def _():
            power, reach = decay[1], decay[4]
            ahead_all, behind_all = slab_moments(moments, i, reach)
            entering = (arrived[i] + power * power * mine[i]) * decay[3]
            turned = halves(entering)
            ahead = jnp.where(lower, turned, halves(ahead_all) + power * entering)
            behind = jnp.where(lower, halves(behind_all) + power * entering, turned)
            edge[0, 0] = ahead
            edge[chunks - 1, 1] = behind
            for k in range(1, chunks):
                ahead = ahead * reach + moments[i, k - 1, 0]
                edge[k, 0] = ahead
                behind = behind * reach + moments[i, chunks - k, 1]
                edge[chunks - 1 - k, 1] = behind

        def chunk_step(c, carry):
            block = pl.ds(pl.multiple_of(c * GROUP, GROUP), GROUP)
            ratio = decay[0]
            scale = decay[2] * number.astype(jnp.float32)
            ahead = edge[c, 0]
            behind = edge[c, 1]
            tails = []
            for k in reversed(range(GROUP)):
                spilled = ratio * behind
                tails.insert(0, spilled)
                behind = spectrum[i, c * GROUP + k] + spilled
            planes = []
            for k in range(GROUP):
                ahead = spectrum[i, c * GROUP + k] + ratio * ahead
                planes.append(scale * (ahead + tails[k]))
            planes = along_second(planes, left_ref[...])
            value = along_last(jnp.concatenate(planes, 0), right_ref[...])
            potential = value.reshape(GROUP, side, width)
            total[i, block] += potential * other[block]
            if inside:
                total[1, block] += potential * own[i, block]
            else:
                partner[block] += potential * own[i, block]
            return carry

        lax.fori_loop(0, jnp.where(number > 0, chunks, 0), chunk_step, 0)
        return carry

    lax.fori_loop(0, owned, orbital_step, 0)


def pair_counts(pair_list, pair_count, owned, band_index, band_count):
    first, partner = pair_list[0, :, 0], pair_list[0, :, 1]
    live = jnp.arange(first.shape[0]) < pair_count[0]
    distance = (partner // owned - band_index) % band_count
    inside = (REACH * owned) * owned
    place = (first * REACH + distance - 1) * owned + partner % owned
    place = jnp.where(distance == 0, inside, place)
    counts = jnp.sum(jnp.where(live, lax.shift_left(1, DIGIT * place), 0)).reshape(1)
    digit = 2**DIGIT - 1
    kept = digit << (DIGIT * inside)
    total = counts & kept
    for distance in range(1, REACH + 1):
        kept = 0
        for k in range(owned * owned):
            spot = (k // owned * REACH + distance - 1) * owned + k % owned
            kept |= digit << (DIGIT * spot)
        total = total | (rotated(counts, "band", distance) & kept)
    return total[0]


def count_at(counts, place):
    return lax.shift_right_logical(counts[0], 1 + DIGIT * place) & (2**DIGIT - 1)


def on_device(orbitals, pair_list, pair_count):
    owned, slab_rows, plane_cells = orbitals.shape
    side = math.isqrt(plane_cells)
    assert lax.axis_size("grid") == 2 and REACH == 2 and owned == 2
    rows = slab_rows // 2
    chunks = rows // GROUP
    band_count = lax.axis_size("band")
    band_index = lax.axis_index("band")
    right, left, decay = tables(side, rows)
    smem = pl.BlockSpec(memory_space=pltpu.SMEM)
    vmem = pl.BlockSpec(memory_space=pltpu.VMEM)
    free = pl.BlockSpec(memory_space=pl.ANY)
    hbm = pl.BlockSpec(memory_space=pltpu.HBM)
    params = pltpu.CompilerParams(vmem_limit_bytes=12 * 2**20)
    shape = (rows, side, 2 * side)
    one = jax.ShapeDtypeStruct(shape, jnp.float32)
    both = jax.ShapeDtypeStruct((owned,) + shape, jnp.float32)

    def call(kernel, out_shape, in_specs, out_specs=vmem, scratch=(), aliases={}):
        if isinstance(out_shape, tuple):
            out_specs = (vmem,) * len(out_shape)
        return pl.pallas_call(
            kernel,
            out_shape=out_shape,
            in_specs=in_specs,
            out_specs=out_specs,
            scratch_shapes=scratch,
            compiler_params=params,
            input_output_aliases=aliases,
            cost_estimate=pl.CostEstimate(flops=0, bytes_accessed=1 << 20, transcendentals=0),
        )

    tiles = tiled(orbitals, 2 * side)
    source = pltpu.with_memory_space_constraint(tiles, pltpu.HBM)
    fields, far = [], []
    for row in range(owned):
        field = call(
            functools.partial(arrange_kernel, row),
            one,
            [hbm] + [free] * row,
            scratch=[
                pltpu.VMEM(tiles.shape[1:], jnp.float32),
                pltpu.SemaphoreType.DMA(tiles.shape[1:2]),
            ],
        )(source, *fields)
        fields.append(field)
        far.append(rotated(field, "band", 2))
    own = call(stack_kernel, both, [vmem, vmem])(*fields)
    flag = (band_index % 2).reshape(1)
    counts = pair_counts(pair_list, pair_count, owned, band_index, band_count)
    counts = (lax.optimization_barrier(counts) * 2 + band_index % 2).reshape(1)

    def forward(base, after, other):
        return call(
            functools.partial(forward_kernel, base),
            (
                both,
                jax.ShapeDtypeStruct((owned, chunks, 2) + shape[1:], jnp.float32),
                jax.ShapeDtypeStruct((owned,) + shape[1:], jnp.float32),
            ),
            [smem, free] + [vmem] * 5,
        )(counts, after, own, other, right, left, decay)

    def exchanged(mine):
        return swapped(mine, "grid")

    def backward(base, after, state, total, inside=False):
        return call(
            functools.partial(backward_kernel, base, inside),
            both if inside else (both, one),
            [smem, free] + [vmem] * (9 + len(total)),
            scratch=[pltpu.VMEM((chunks, 2) + shape[1:], jnp.float32)],
        )(counts, after, own, *state, right, left, decay, *total)

    inner_base = REACH * owned * owned
    spectrum, moments, mine = forward(inner_base, own, fields[1])
    inner = (fields[1], spectrum, moments, mine, exchanged(mine))
    after = mine

    def brought(row, after):
        picked = call(pick_kernel, one, [smem, free, vmem, vmem])(
            flag, after, fields[row], far[row]
        )
        return picked, swapped(picked, "band")

    total, passed, arrived = (), [], []
    after, near = brought(0, after)
    for row in range(owned):
        base = row * REACH * owned
        distant_state = forward(base + owned, after, far[row])
        distant_ends = exchanged(distant_state[2])
        near_state = forward(base, distant_state[2], near)
        mine = near_state[2]
        near_state = (near,) + tuple(near_state) + (exchanged(mine),)
        distant_state = (far[row],) + tuple(distant_state) + (distant_ends,)
        acc, handed = backward(base, mine, near_state, total)
        handed_over = swapped(handed, "band")
        acc, distant = backward(base + owned, handed, distant_state, (acc,))
        total = (acc,)
        joined = call(join_kernel, one, [smem, free, vmem, vmem])(
            flag, distant, distant, handed_over
        )
        passed.append(handed_over)
        arrived.append(rotated(joined, "band", -2))
        after = joined
        if row + 1 < owned:
            after, near = brought(row + 1, joined)
    total = backward(inner_base, after, inner, total, inside=True)
    out = jax.ShapeDtypeStruct(tiles.shape, jnp.float32)
    result = None
    for row in range(owned):
        earlier = [] if result is None else [result]
        result = call(
            functools.partial(restore_kernel, row),
            out,
            [smem] + [vmem] * 3 + [hbm] * len(earlier),
            out_specs=hbm,
            scratch=[
                pltpu.VMEM(tiles.shape[1:], jnp.float32),
                pltpu.SemaphoreType.DMA(tiles.shape[1:2]),
            ],
            aliases={4: 0} if earlier else {},
        )(flag, total, passed[row], arrived[row], *earlier)
    return jnp.transpose(result, (0, 1, 3, 2, 4)).reshape(orbitals.shape)


def solution(mesh):
    in_specs = (P("band", "grid", None), P("band", None, None), P("band"))
    out_specs = P("band", "grid", None)

    return jax.shard_map(
        on_device, mesh=mesh, in_specs=in_specs, out_specs=out_specs, check_vma=False
    )
```

```python
import functools
import math

import jax
import jax.numpy as jnp
import numpy as np
from jax import lax
from jax.experimental import pallas as pl
from jax.experimental.pallas import tpu as pltpu
from jax.sharding import PartitionSpec as P

REACH = 2
GROUP = 8


def rotated(value, axis, steps):
    count = lax.axis_size(axis)
    pairs = [(source, (source + steps) % count) for source in range(count)]
    return lax.ppermute(value, axis, pairs)


def swapped(value, axis):
    count = lax.axis_size(axis)
    return lax.ppermute(value, axis, [(source, source ^ 1) for source in range(count)])


def split(value):
    high = value.astype(jnp.bfloat16)
    return high, (value - high.astype(jnp.float32)).astype(jnp.bfloat16)


def tables(side, half_rows):
    points = np.arange(side)
    angles = (points[:, None] * points[None, :] % side) * (2.0 * math.pi / side)
    hartley = (np.cos(angles) + np.sin(angles)).astype(np.float32)
    high = hartley.astype(jnp.bfloat16)
    low = (hartley - high.astype(np.float32)).astype(jnp.bfloat16)
    eye = np.eye(2, dtype=np.float32)
    wide_high = np.kron(eye, high.astype(np.float32))
    wide_low = np.kron(eye, low.astype(np.float32))
    right = np.block([[wide_high, wide_low], [wide_high, wide_low]]).astype(jnp.bfloat16)
    order = np.concatenate([points[0::2], points[1::2]])
    left = np.concatenate([part[order][:, order] for part in (high, high, low)], 1)
    eigenvalues = 2.0 - 2.0 * np.cos(points * (2.0 * math.pi / side))
    shift = 1.0 / side**2 + eigenvalues[order][:, None] + np.tile(eigenvalues, 2)[None, :]
    ratio = 1.0 + shift / 2 - np.sqrt(shift + shift**2 / 4)
    power = ratio**half_rows
    reach = ratio**GROUP
    scale = 1.0 / side / (1.0 / ratio - ratio) / side**2
    wrap = 1.0 / (1.0 - power**4)
    decay = np.stack([ratio, power, scale, wrap, reach]).astype(np.float32)
    return right, left, decay


def along_last(value, right):
    width = value.shape[1]
    product = jnp.dot(
        jnp.concatenate(split(value), 1), right, preferred_element_type=jnp.float32
    )
    return product[:, :width] + product[:, width:]


def along_second(planes, left):
    width = planes[0].shape[1]
    out = []
    for start in range(0, len(planes), 2):
        both = jnp.concatenate(planes[start : start + 2], 1)
        high, low = split(both)
        stacked = jnp.concatenate([high, low, high], 0)
        product = jnp.dot(left, stacked, preferred_element_type=jnp.float32)
        out.append(product[:, :width])
        out.append(product[:, width:])
    return out


def halves(value):
    return pltpu.roll(value, value.shape[-1] // 2, axis=value.ndim - 1)


DIGIT = 3


def tiled(value, width):
    count, slab_rows, cells = value.shape
    value = value.reshape(count, slab_rows // GROUP, GROUP, cells // width, width)
    return jnp.transpose(value, (0, 1, 3, 2, 4))


def arrange_kernel(row, source, *refs):
    packed, raw, arrivals = refs[-3:]
    groups, tiles, lines, width = raw.shape
    flat = raw.reshape(groups * tiles * lines, width)
    lower = lax.broadcasted_iota(jnp.int32, (tiles, width), 1) < width // 2
    half = groups // 2
    copies = [
        pltpu.make_async_copy(source.at[row, g], raw.at[g], arrivals.at[g]) for g in range(groups)
    ]
    for g in range(half):
        copies[g].start()
        copies[g + half].start()
    for g in range(half):
        copies[g].wait()
        copies[g + half].wait()
        for k in range(lines):
            near = flat[pl.ds(g * tiles * lines + k, tiles, stride=lines), :]
            far = flat[pl.ds((g + half) * tiles * lines + k, tiles, stride=lines), :]
            packed[g * lines + k, :tiles] = jnp.where(lower, near, halves(far))
            packed[g * lines + k, tiles:] = jnp.where(lower, halves(near), far)


def stack_kernel(first, second, own):
    own[0] = first[...]
    own[1] = second[...]


def restore_kernel(row, flag, own, passed, arrived, *refs):
    out, raw, departures = refs[-3:]
    groups, tiles, lines, width = raw.shape
    flat = raw.reshape(groups * tiles * lines, width)
    lower = lax.broadcasted_iota(jnp.int32, (tiles, width), 1) < width // 2
    half = groups // 2
    weight = 1.0 - flag[0].astype(jnp.float32)
    copies = [
        pltpu.make_async_copy(raw.at[g], out.at[row, g], departures.at[g]) for g in range(groups)
    ]
    for g in range(half):
        for k in range(lines):
            plane = g * lines + k
            block = own[row, plane] + weight * passed[plane] + arrived[plane]
            even, odd = block[:tiles], block[tiles:]
            near = pl.ds(g * tiles * lines + k, tiles, stride=lines)
            far = pl.ds((g + half) * tiles * lines + k, tiles, stride=lines)
            flat[near, :] = jnp.where(lower, even, halves(odd))
            flat[far, :] = jnp.where(lower, halves(even), odd)
        copies[g].start()
        copies[g + half].start()
    for copy in copies:
        copy.wait()


def pick_kernel(flag, after, own, far, out):
    @pl.when(flag[0] == 0)
    def _():
        out[...] = own[...]

    @pl.when(flag[0] == 1)
    def _():
        out[...] = far[...]


def join_kernel(flag, after, distant, handed, out):
    weight = flag[0].astype(jnp.float32)
    out[...] = distant[...] + weight * handed[...]


def slab_moments(moments, i, reach):
    count = moments.shape[1]
    ahead = moments[i, 0, 0]
    behind = moments[i, count - 1, 1]
    for k in range(1, count):
        ahead = ahead * reach + moments[i, k, 0]
        behind = behind * reach + moments[i, count - 1 - k, 1]
    return ahead, behind


def forward_kernel(base, counts, after, own, other, right_ref, left_ref, decay, *refs):
    spectrum, moments, mine = refs
    owned, rows, side, width = own.shape
    chunks = rows // GROUP
    lower = lax.broadcasted_iota(jnp.int32, (side, width), 1) < width // 2

    def orbital_step(i, carry):
        live = count_at(counts, base + i) > 0

        def chunk_step(c, carry):
            block = pl.ds(pl.multiple_of(c * GROUP, GROUP), GROUP)
            density = own[i, block] * other[block]
            value = along_last(density.reshape(GROUP * side, width), right_ref[...])
            planes = [value[k * side : (k + 1) * side] for k in range(GROUP)]
            planes = along_second(planes, left_ref[...])
            ratio = decay[0]
            ahead = planes[0]
            behind = planes[-1]
            for k in range(GROUP):
                spectrum[i, c * GROUP + k] = planes[k]
                if k:
                    ahead = ahead * ratio + planes[k]
                    behind = behind * ratio + planes[GROUP - 1 - k]
            moments[i, c, 0] = ahead
            moments[i, c, 1] = behind
            return carry

        lax.fori_loop(0, jnp.where(live, chunks, 0), chunk_step, 0)

        @pl.when(live)
        def _():
            power = decay[1]
            ahead, behind = slab_moments(moments, i, decay[4])
            mine[i] = jnp.where(lower, behind + power * halves(behind), ahead + power * halves(ahead))

        return carry

    lax.fori_loop(0, owned, orbital_step, 0)


def backward_kernel(
    base, inside, counts, after, own, other, spectrum, moments, mine, arrived,
    right_ref, left_ref, decay, *refs
):
    edge = refs[-1]
    if inside:
        before, total = refs[:2]
        total[...] = before[...]
    else:
        total, partner = refs[-3:-1]
        total[...] = refs[0][...] if len(refs) > 3 else jnp.zeros_like(total)
        partner[...] = jnp.zeros_like(partner)
    owned, rows, side, width = own.shape
    chunks = rows // GROUP
    lower = lax.broadcasted_iota(jnp.int32, (side, width), 1) < width // 2

    def orbital_step(i, carry):
        number = count_at(counts, base + i)

        @pl.when(number > 0)
        def _():
            power, reach = decay[1], decay[4]
            ahead_all, behind_all = slab_moments(moments, i, reach)
            entering = (arrived[i] + power * power * mine[i]) * decay[3]
            turned = halves(entering)
            ahead = jnp.where(lower, turned, halves(ahead_all) + power * entering)
            behind = jnp.where(lower, halves(behind_all) + power * entering, turned)
            edge[0, 0] = ahead
            edge[chunks - 1, 1] = behind
            for k in range(1, chunks):
                ahead = ahead * reach + moments[i, k - 1, 0]
                edge[k, 0] = ahead
                behind = behind * reach + moments[i, chunks - k, 1]
                edge[chunks - 1 - k, 1] = behind

        def chunk_step(c, carry):
            block = pl.ds(pl.multiple_of(c * GROUP, GROUP), GROUP)
            ratio = decay[0]
            scale = decay[2] * number.astype(jnp.float32)
            ahead = edge[c, 0]
            behind = edge[c, 1]
            tails = []
            for k in reversed(range(GROUP)):
                spilled = ratio * behind
                tails.insert(0, spilled)
                behind = spectrum[i, c * GROUP + k] + spilled
            planes = []
            for k in range(GROUP):
                ahead = spectrum[i, c * GROUP + k] + ratio * ahead
                planes.append(scale * (ahead + tails[k]))
            planes = along_second(planes, left_ref[...])
            value = along_last(jnp.concatenate(planes, 0), right_ref[...])
            potential = value.reshape(GROUP, side, width)
            total[i, block] += potential * other[block]
            if inside:
                total[1, block] += potential * own[i, block]
            else:
                partner[block] += potential * own[i, block]
            return carry

        lax.fori_loop(0, jnp.where(number > 0, chunks, 0), chunk_step, 0)
        return carry

    lax.fori_loop(0, owned, orbital_step, 0)


def pair_counts(pair_list, pair_count, owned, band_index, band_count):
    first, partner = pair_list[0, :, 0], pair_list[0, :, 1]
    live = jnp.arange(first.shape[0]) < pair_count[0]
    distance = (partner // owned - band_index) % band_count
    inside = (REACH * owned) * owned
    place = (first * REACH + distance - 1) * owned + partner % owned
    place = jnp.where(distance == 0, inside, place)
    counts = jnp.sum(jnp.where(live, lax.shift_left(1, DIGIT * place), 0)).reshape(1)
    digit = 2**DIGIT - 1
    total = jnp.int32(0)
    for distance in range(1, REACH + 1):
        kept = 0
        for k in range(owned * owned):
            spot = (k // owned * REACH + distance - 1) * owned + k % owned
            kept |= digit << (DIGIT * spot)
        total = total | (lax.optimization_barrier(rotated(counts, "band", distance)[0]) & kept)
    return counts[0], total


def count_at(counts, place):
    return lax.shift_right_logical(counts[0], 1 + DIGIT * place) & (2**DIGIT - 1)


def on_device(orbitals, pair_list, pair_count):
    owned, slab_rows, plane_cells = orbitals.shape
    side = math.isqrt(plane_cells)
    assert lax.axis_size("grid") == 2 and REACH == 2 and owned == 2
    rows = slab_rows // 2
    chunks = rows // GROUP
    band_count = lax.axis_size("band")
    band_index = lax.axis_index("band")
    right, left, decay = tables(side, rows)
    smem = pl.BlockSpec(memory_space=pltpu.SMEM)
    vmem = pl.BlockSpec(memory_space=pltpu.VMEM)
    free = pl.BlockSpec(memory_space=pl.ANY)
    hbm = pl.BlockSpec(memory_space=pltpu.HBM)
    params = pltpu.CompilerParams(vmem_limit_bytes=12 * 2**20)
    shape = (rows, side, 2 * side)
    one = jax.ShapeDtypeStruct(shape, jnp.float32)
    both = jax.ShapeDtypeStruct((owned,) + shape, jnp.float32)

    def call(kernel, out_shape, in_specs, out_specs=vmem, scratch=(), aliases={}):
        if isinstance(out_shape, tuple):
            out_specs = (vmem,) * len(out_shape)
        return pl.pallas_call(
            kernel,
            out_shape=out_shape,
            in_specs=in_specs,
            out_specs=out_specs,
            scratch_shapes=scratch,
            compiler_params=params,
            input_output_aliases=aliases,
            cost_estimate=pl.CostEstimate(flops=0, bytes_accessed=1 << 20, transcendentals=0),
        )

    tiles = tiled(orbitals, 2 * side)
    source = pltpu.with_memory_space_constraint(tiles, pltpu.HBM)
    fields, far = [], []
    for row in range(owned):
        field = call(
            functools.partial(arrange_kernel, row),
            one,
            [hbm] + [free] * row,
            scratch=[
                pltpu.VMEM(tiles.shape[1:], jnp.float32),
                pltpu.SemaphoreType.DMA(tiles.shape[1:2]),
            ],
        )(source, *fields)
        fields.append(field)
        far.append(rotated(field, "band", 2))
    own = call(stack_kernel, both, [vmem, vmem])(*fields)
    flag = (band_index % 2).reshape(1)
    listed, counts = pair_counts(pair_list, pair_count, owned, band_index, band_count)
    listed = (lax.optimization_barrier(listed) * 2 + band_index % 2).reshape(1)
    counts = (counts * 2 + band_index % 2).reshape(1)

    def forward(base, after, other, counts=counts):
        return call(
            functools.partial(forward_kernel, base),
            (
                both,
                jax.ShapeDtypeStruct((owned, chunks, 2) + shape[1:], jnp.float32),
                jax.ShapeDtypeStruct((owned,) + shape[1:], jnp.float32),
            ),
            [smem, free] + [vmem] * 5,
        )(counts, after, own, other, right, left, decay)

    def exchanged(mine):
        return swapped(mine, "grid")

    def backward(base, after, state, total, inside=False):
        numbers = listed if inside else counts
        return call(
            functools.partial(backward_kernel, base, inside),
            both if inside else (both, one),
            [smem, free] + [vmem] * (9 + len(total)),
            scratch=[pltpu.VMEM((chunks, 2) + shape[1:], jnp.float32)],
        )(numbers, after, own, *state, right, left, decay, *total)

    inner_base = REACH * owned * owned
    spectrum, moments, mine = forward(inner_base, own, fields[1], listed)
    inner = (fields[1], spectrum, moments, mine, exchanged(mine))
    after = mine

    def brought(row, after):
        picked = call(pick_kernel, one, [smem, free, vmem, vmem])(
            flag, after, fields[row], far[row]
        )
        return picked, swapped(picked, "band")

    total, passed, arrived = (), [], []
    after, near = brought(0, after)
    for row in range(owned):
        base = row * REACH * owned
        distant_state = forward(base + owned, after, far[row])
        distant_ends = exchanged(distant_state[2])
        near_state = forward(base, distant_state[2], near)
        mine = near_state[2]
        near_state = (near,) + tuple(near_state) + (exchanged(mine),)
        distant_state = (far[row],) + tuple(distant_state) + (distant_ends,)
        acc, handed = backward(base, mine, near_state, total)
        handed_over = swapped(handed, "band")
        acc, distant = backward(base + owned, handed, distant_state, (acc,))
        total = (acc,)
        joined = call(join_kernel, one, [smem, free, vmem, vmem])(
            flag, distant, distant, handed_over
        )
        passed.append(handed_over)
        arrived.append(rotated(joined, "band", -2))
        after = joined
        if row + 1 < owned:
            after, near = brought(row + 1, joined)
    total = backward(inner_base, after, inner, total, inside=True)
    out = jax.ShapeDtypeStruct(tiles.shape, jnp.float32)
    result = None
    for row in range(owned):
        earlier = [] if result is None else [result]
        result = call(
            functools.partial(restore_kernel, row),
            out,
            [smem] + [vmem] * 3 + [hbm] * len(earlier),
            out_specs=hbm,
            scratch=[
                pltpu.VMEM(tiles.shape[1:], jnp.float32),
                pltpu.SemaphoreType.DMA(tiles.shape[1:2]),
            ],
            aliases={4: 0} if earlier else {},
        )(flag, total, passed[row], arrived[row], *earlier)
    return jnp.transpose(result, (0, 1, 3, 2, 4)).reshape(orbitals.shape)


def solution(mesh):
    in_specs = (P("band", "grid", None), P("band", None, None), P("band"))
    out_specs = P("band", "grid", None)

    return jax.shard_map(
        on_device, mesh=mesh, in_specs=in_specs, out_specs=out_specs, check_vma=False
    )
```

```python
import functools
import math

import jax
import jax.numpy as jnp
import numpy as np
from jax import lax
from jax.experimental import pallas as pl
from jax.experimental.pallas import tpu as pltpu
from jax.sharding import PartitionSpec as P

REACH = 2
GROUP = 8


def rotated(value, axis, steps):
    count = lax.axis_size(axis)
    pairs = [(source, (source + steps) % count) for source in range(count)]
    return lax.ppermute(value, axis, pairs)


def swapped(value, axis):
    count = lax.axis_size(axis)
    return lax.ppermute(value, axis, [(source, source ^ 1) for source in range(count)])


def split(value):
    high = value.astype(jnp.bfloat16)
    return high, (value - high.astype(jnp.float32)).astype(jnp.bfloat16)


def tables(side, half_rows):
    points = np.arange(side)
    angles = (points[:, None] * points[None, :] % side) * (2.0 * math.pi / side)
    hartley = (np.cos(angles) + np.sin(angles)).astype(np.float32)
    high = hartley.astype(jnp.bfloat16)
    low = (hartley - high.astype(np.float32)).astype(jnp.bfloat16)
    eye = np.eye(2, dtype=np.float32)
    wide_high = np.kron(eye, high.astype(np.float32))
    wide_low = np.kron(eye, low.astype(np.float32))
    right = np.block([[wide_high, wide_low], [wide_high, wide_low]]).astype(jnp.bfloat16)
    order = np.concatenate([points[0::2], points[1::2]])
    left = np.concatenate([part[order][:, order] for part in (high, high, low)], 1)
    eigenvalues = 2.0 - 2.0 * np.cos(points * (2.0 * math.pi / side))
    shift = 1.0 / side**2 + eigenvalues[order][:, None] + np.tile(eigenvalues, 2)[None, :]
    ratio = 1.0 + shift / 2 - np.sqrt(shift + shift**2 / 4)
    power = ratio**half_rows
    reach = ratio**GROUP
    scale = 1.0 / side / (1.0 / ratio - ratio) / side**2
    wrap = 1.0 / (1.0 - power**4)
    decay = np.stack([ratio, power, scale, wrap, reach]).astype(np.float32)
    return right, left, decay


def along_last(value, right):
    width = value.shape[1]
    product = jnp.dot(
        jnp.concatenate(split(value), 1), right, preferred_element_type=jnp.float32
    )
    return product[:, :width] + product[:, width:]


def along_second(planes, left):
    width = planes[0].shape[1]
    out = []
    for start in range(0, len(planes), 2):
        both = jnp.concatenate(planes[start : start + 2], 1)
        high, low = split(both)
        stacked = jnp.concatenate([high, low, high], 0)
        product = jnp.dot(left, stacked, preferred_element_type=jnp.float32)
        out.append(product[:, :width])
        out.append(product[:, width:])
    return out


def halves(value):
    return pltpu.roll(value, value.shape[-1] // 2, axis=value.ndim - 1)


DIGIT = 3


def tiled(value, width):
    count, slab_rows, cells = value.shape
    value = value.reshape(count, slab_rows // GROUP, GROUP, cells // width, width)
    return jnp.transpose(value, (0, 1, 3, 2, 4))


def arrange_kernel(row, source, *refs):
    packed, raw, arrivals = refs[-3:]
    groups, tiles, lines, width = raw.shape
    flat = raw.reshape(groups * tiles * lines, width)
    lower = lax.broadcasted_iota(jnp.int32, (tiles, width), 1) < width // 2
    half = groups // 2
    copies = [
        pltpu.make_async_copy(source.at[row, g], raw.at[g], arrivals.at[g]) for g in range(groups)
    ]
    for g in range(half):
        copies[g].start()
        copies[g + half].start()
    for g in range(half):
        copies[g].wait()
        copies[g + half].wait()
        for k in range(lines):
            near = flat[pl.ds(g * tiles * lines + k, tiles, stride=lines), :]
            far = flat[pl.ds((g + half) * tiles * lines + k, tiles, stride=lines), :]
            packed[g * lines + k, :tiles] = jnp.where(lower, near, halves(far))
            packed[g * lines + k, tiles:] = jnp.where(lower, halves(near), far)


def stack_kernel(first, second, own):
    own[0] = first[...]
    own[1] = second[...]


def restore_kernel(row, flag, own, passed, arrived, *refs):
    out, raw, departures = refs[-3:]
    groups, tiles, lines, width = raw.shape
    flat = raw.reshape(groups * tiles * lines, width)
    lower = lax.broadcasted_iota(jnp.int32, (tiles, width), 1) < width // 2
    half = groups // 2
    weight = 1.0 - flag[0].astype(jnp.float32)
    copies = [
        pltpu.make_async_copy(raw.at[g], out.at[row, g], departures.at[g]) for g in range(groups)
    ]
    for g in range(half):
        for k in range(lines):
            plane = g * lines + k
            block = own[row, plane] + weight * passed[plane] + arrived[plane]
            even, odd = block[:tiles], block[tiles:]
            near = pl.ds(g * tiles * lines + k, tiles, stride=lines)
            far = pl.ds((g + half) * tiles * lines + k, tiles, stride=lines)
            flat[near, :] = jnp.where(lower, even, halves(odd))
            flat[far, :] = jnp.where(lower, halves(even), odd)
        copies[g].start()
        copies[g + half].start()
    for copy in copies:
        copy.wait()


def pick_kernel(flag, after, own, far, out):
    @pl.when(flag[0] & 1 == 0)
    def _():
        out[...] = own[...]

    @pl.when(flag[0] & 1 == 1)
    def _():
        out[...] = far[...]


def join_kernel(flag, after, distant, handed, out):
    weight = flag[0].astype(jnp.float32)
    out[...] = distant[...] + weight * handed[...]


def slab_moments(moments, i, reach):
    count = moments.shape[1]
    ahead = moments[i, 0, 0]
    behind = moments[i, count - 1, 1]
    for k in range(1, count):
        ahead = ahead * reach + moments[i, k, 0]
        behind = behind * reach + moments[i, count - 1 - k, 1]
    return ahead, behind


def forward_kernel(base, counts, after, own, other, right_ref, left_ref, decay, *refs):
    spectrum, moments, mine = refs
    _, rows, side, width = own.shape
    chunks = rows // GROUP
    lower = lax.broadcasted_iota(jnp.int32, (side, width), 1) < width // 2

    def orbital_step(i, carry):
        live = count_at(counts, base + i) > 0

        def chunk_step(c, carry):
            block = pl.ds(pl.multiple_of(c * GROUP, GROUP), GROUP)
            density = own[i, block] * other[block]
            value = along_last(density.reshape(GROUP * side, width), right_ref[...])
            planes = [value[k * side : (k + 1) * side] for k in range(GROUP)]
            planes = along_second(planes, left_ref[...])
            ratio = decay[0]
            ahead = planes[0]
            behind = planes[-1]
            for k in range(GROUP):
                spectrum[i, c * GROUP + k] = planes[k]
                if k:
                    ahead = ahead * ratio + planes[k]
                    behind = behind * ratio + planes[GROUP - 1 - k]
            moments[i, c, 0] = ahead
            moments[i, c, 1] = behind
            return carry

        lax.fori_loop(0, jnp.where(live, chunks, 0), chunk_step, 0)

        @pl.when(live)
        def _():
            power = decay[1]
            ahead, behind = slab_moments(moments, i, decay[4])
            mine[i] = jnp.where(lower, behind + power * halves(behind), ahead + power * halves(ahead))

        return carry

    lax.fori_loop(0, spectrum.shape[0], orbital_step, 0)


def backward_kernel(
    base, inside, counts, after, own, other, spectrum, moments, mine, arrived,
    right_ref, left_ref, decay, *refs
):
    edge = refs[-1]
    if inside:
        before, total = refs[:2]
        total[...] = before[...]
    else:
        total, partner = refs[-3:-1]
        total[...] = refs[0][...] if len(refs) > 3 else jnp.zeros_like(total)
        partner[...] = jnp.zeros_like(partner)
    _, rows, side, width = own.shape
    chunks = rows // GROUP
    lower = lax.broadcasted_iota(jnp.int32, (side, width), 1) < width // 2

    def orbital_step(i, carry):
        number = count_at(counts, base + i)

        @pl.when(number > 0)
        def _():
            power, reach = decay[1], decay[4]
            ahead_all, behind_all = slab_moments(moments, i, reach)
            entering = (arrived[i] + power * power * mine[i]) * decay[3]
            turned = halves(entering)
            ahead = jnp.where(lower, turned, halves(ahead_all) + power * entering)
            behind = jnp.where(lower, halves(behind_all) + power * entering, turned)
            edge[0, 0] = ahead
            edge[chunks - 1, 1] = behind
            for k in range(1, chunks):
                ahead = ahead * reach + moments[i, k - 1, 0]
                edge[k, 0] = ahead
                behind = behind * reach + moments[i, chunks - k, 1]
                edge[chunks - 1 - k, 1] = behind

        def chunk_step(c, carry):
            block = pl.ds(pl.multiple_of(c * GROUP, GROUP), GROUP)
            ratio = decay[0]
            scale = decay[2] * number.astype(jnp.float32)
            ahead = edge[c, 0]
            behind = edge[c, 1]
            tails = []
            for k in reversed(range(GROUP)):
                spilled = ratio * behind
                tails.insert(0, spilled)
                behind = spectrum[i, c * GROUP + k] + spilled
            planes = []
            for k in range(GROUP):
                ahead = spectrum[i, c * GROUP + k] + ratio * ahead
                planes.append(scale * (ahead + tails[k]))
            planes = along_second(planes, left_ref[...])
            value = along_last(jnp.concatenate(planes, 0), right_ref[...])
            potential = value.reshape(GROUP, side, width)
            total[i, block] += potential * other[block]
            if inside:
                total[1, block] += potential * own[i, block]
            else:
                partner[block] += potential * own[i, block]
            return carry

        lax.fori_loop(0, jnp.where(number > 0, chunks, 0), chunk_step, 0)
        return carry

    lax.fori_loop(0, spectrum.shape[0], orbital_step, 0)


def pair_counts(pair_list, pair_count, owned, band_index, band_count):
    first, partner = pair_list[0, :, 0], pair_list[0, :, 1]
    live = jnp.arange(first.shape[0]) < pair_count[0]
    distance = (partner // owned - band_index) % band_count
    inside = (REACH * owned) * owned
    place = (first * REACH + distance - 1) * owned + partner % owned
    place = jnp.where(distance == 0, inside, place)
    counts = jnp.sum(jnp.where(live, lax.shift_left(1, DIGIT * place), 0)).reshape(1)
    digit = 2**DIGIT - 1
    total = jnp.int32(0)
    for distance in range(1, REACH + 1):
        kept = 0
        for k in range(owned * owned):
            spot = (k // owned * REACH + distance - 1) * owned + k % owned
            kept |= digit << (DIGIT * spot)
        total = total | (lax.optimization_barrier(rotated(counts, "band", distance)[0]) & kept)
    return counts[0], total


def count_at(counts, place):
    return lax.shift_right_logical(counts[0], 1 + DIGIT * place) & (2**DIGIT - 1)


def on_device(orbitals, pair_list, pair_count):
    owned, slab_rows, plane_cells = orbitals.shape
    side = math.isqrt(plane_cells)
    assert lax.axis_size("grid") == 2 and REACH == 2 and owned == 2
    rows = slab_rows // 2
    chunks = rows // GROUP
    band_count = lax.axis_size("band")
    band_index = lax.axis_index("band")
    right, left, decay = tables(side, rows)
    smem = pl.BlockSpec(memory_space=pltpu.SMEM)
    vmem = pl.BlockSpec(memory_space=pltpu.VMEM)
    free = pl.BlockSpec(memory_space=pl.ANY)
    hbm = pl.BlockSpec(memory_space=pltpu.HBM)
    params = pltpu.CompilerParams(vmem_limit_bytes=12 * 2**20)
    shape = (rows, side, 2 * side)
    one = jax.ShapeDtypeStruct(shape, jnp.float32)
    both = jax.ShapeDtypeStruct((owned,) + shape, jnp.float32)

    def call(kernel, out_shape, in_specs, out_specs=vmem, scratch=(), aliases={}):
        if isinstance(out_shape, tuple):
            out_specs = (vmem,) * len(out_shape)
        return pl.pallas_call(
            kernel,
            out_shape=out_shape,
            in_specs=in_specs,
            out_specs=out_specs,
            scratch_shapes=scratch,
            compiler_params=params,
            input_output_aliases=aliases,
            cost_estimate=pl.CostEstimate(flops=0, bytes_accessed=1 << 20, transcendentals=0),
        )

    tiles = tiled(orbitals, 2 * side)
    source = pltpu.with_memory_space_constraint(tiles, pltpu.HBM)
    fields, far = [], []
    for row in range(owned):
        field = call(
            functools.partial(arrange_kernel, row),
            one,
            [hbm] + [free] * row,
            scratch=[
                pltpu.VMEM(tiles.shape[1:], jnp.float32),
                pltpu.SemaphoreType.DMA(tiles.shape[1:2]),
            ],
        )(source, *fields)
        fields.append(field)
        far.append(rotated(field, "band", 2))
    own = call(stack_kernel, both, [vmem, vmem])(*fields)
    flag = (band_index % 2).reshape(1)
    listed, counts = pair_counts(pair_list, pair_count, owned, band_index, band_count)
    listed = (lax.optimization_barrier(listed) * 2 + band_index % 2).reshape(1)
    counts = (counts * 2 + band_index % 2).reshape(1)

    def forward(base, after, other, counts=counts, inside=False):
        lines = (1 if inside else owned,)
        return call(
            functools.partial(forward_kernel, base),
            (
                jax.ShapeDtypeStruct(lines + shape, jnp.float32),
                jax.ShapeDtypeStruct(lines + (chunks, 2) + shape[1:], jnp.float32),
                jax.ShapeDtypeStruct(lines + shape[1:], jnp.float32),
            ),
            [smem, free] + [vmem] * 5,
        )(counts, after, own, other, right, left, decay)

    def exchanged(mine):
        return swapped(mine, "grid")

    def backward(base, after, state, total, inside=False):
        numbers = listed if inside else counts
        return call(
            functools.partial(backward_kernel, base, inside),
            both if inside else (both, one),
            [smem, free] + [vmem] * (9 + len(total)),
            scratch=[pltpu.VMEM((chunks, 2) + shape[1:], jnp.float32)],
        )(numbers, after, own, *state, right, left, decay, *total)

    inner_base = REACH * owned * owned
    spectrum, moments, mine = forward(inner_base, own, fields[1], listed, inside=True)
    inner = (fields[1], spectrum, moments, mine, exchanged(mine))
    after = mine

    def brought(row, after):
        picked = call(pick_kernel, one, [smem, free, vmem, vmem])(
            counts, after, fields[row], far[row]
        )
        return picked, swapped(picked, "band")

    total, passed, arrived = (), [], []
    after, near = brought(0, after)
    for row in range(owned):
        base = row * REACH * owned
        distant_state = forward(base + owned, after, far[row])
        distant_ends = exchanged(distant_state[2])
        near_state = forward(base, distant_state[2], near)
        mine = near_state[2]
        near_state = (near,) + tuple(near_state) + (exchanged(mine),)
        distant_state = (far[row],) + tuple(distant_state) + (distant_ends,)
        acc, handed = backward(base, mine, near_state, total)
        handed_over = swapped(handed, "band")
        acc, distant = backward(base + owned, handed, distant_state, (acc,))
        total = (acc,)
        joined = call(join_kernel, one, [smem, free, vmem, vmem])(
            flag, distant, distant, handed_over
        )
        passed.append(handed_over)
        arrived.append(rotated(joined, "band", -2))
        after = joined
        if row + 1 < owned:
            after, near = brought(row + 1, joined)
    total = backward(inner_base, after, inner, total, inside=True)
    out = jax.ShapeDtypeStruct(tiles.shape, jnp.float32)
    result = None
    for row in range(owned):
        earlier = [] if result is None else [result]
        result = call(
            functools.partial(restore_kernel, row),
            out,
            [smem] + [vmem] * 3 + [hbm] * len(earlier),
            out_specs=hbm,
            scratch=[
                pltpu.VMEM(tiles.shape[1:], jnp.float32),
                pltpu.SemaphoreType.DMA(tiles.shape[1:2]),
            ],
            aliases={4: 0} if earlier else {},
        )(flag, total, passed[row], arrived[row], *earlier)
    return jnp.transpose(result, (0, 1, 3, 2, 4)).reshape(orbitals.shape)


def solution(mesh):
    in_specs = (P("band", "grid", None), P("band", None, None), P("band"))
    out_specs = P("band", "grid", None)

    return jax.shard_map(
        on_device, mesh=mesh, in_specs=in_specs, out_specs=out_specs, check_vma=False
    )
```
